32 devices in a mesh: dp: 1 (over z), ing: 4 (over y), grp: 8 (over x, core).
Axes of the slice: x: 4, y: 4, z: 1, core: 2. Of those that a mesh axis runs over, the one named last changes fastest.
The devices are a block of a 4x4x8 slice.
Arguments:
- tokens: bfloat16 [4096, 2560], P(('dp', 'grp', 'ing'))
- expert_ids: int32 [4096, 3, 2], P(('dp', 'grp', 'ing'))
- gate_vals: float32 [4096, 3, 2], P(('dp', 'grp', 'ing'))
- w_one: bfloat16 [64, 2560, 1536], P(('grp', 'ing'))
- w_three: bfloat16 [64, 2560, 1536], P(('grp', 'ing'))
- w_two: bfloat16 [64, 1536, 2560], P(('grp', 'ing'))
Outputs:
- output: bfloat16 [4096, 2560], P(('dp', 'grp', 'ing'))
All inputs are finite; a program needn't handle non-finite values.
Results may differ from the reference program's by a relative error of at most 0.00128.
Values are sent between devices in bfloat16 or wider.
A program may use at most 768 MiB of HBM per device.

```python
import jax
import jax.numpy as jnp
from jax import lax

TOK = 128
D = 2560
FF = 1536
EXPERTS = 64
TOP = 6
TOPG = 3
GRP = 8
ING = 4

DEVS = GRP * ING
ROWS = DEVS * TOK
M_GROUPS = min(TOPG, GRP // 2)
PER_GROUP = TOP // M_GROUPS
EXP_GROUP = EXPERTS // GRP
CAP_GROUP = (TOK * M_GROUPS + GRP - 1) // GRP
CAP_EXP = (CAP_GROUP * PER_GROUP + EXP_GROUP - 1) // EXP_GROUP
EXP_ROWS = DEVS * CAP_EXP


def draw_routing(route_key):
    key_perm, key_off, key_gperm, key_eoff, key_eperm = jax.random.split(route_key, 5)
    dev_ids = jnp.arange(DEVS)[:, None, None]
    tok_order = jax.vmap(lambda sub_key: jax.random.permutation(sub_key, TOK))(jax.random.split(key_perm, DEVS))
    grp_perm = jax.vmap(lambda sub_key: jax.random.permutation(sub_key, GRP))(jax.random.split(key_gperm, DEVS))
    exp_perm = jax.vmap(lambda sub_key: jax.random.permutation(sub_key, EXP_GROUP))(jax.random.split(key_eperm, DEVS * GRP)).reshape(DEVS, GRP, EXP_GROUP)
    grp_off = jax.random.randint(key_off, (DEVS, 1, 1), 0, GRP)
    exp_off = jax.random.randint(key_eoff, (DEVS, GRP), 0, EXP_GROUP)
    order_pos = jnp.arange(TOK)[:, None] * M_GROUPS + jnp.arange(M_GROUPS)[None, :]
    residue = (order_pos[None, :, :] + grp_off) % GRP
    res_count = jnp.sum((residue[..., None] == jnp.arange(GRP)).astype(jnp.int32), axis=2)
    earlier = jnp.cumsum(res_count, axis=1) - res_count
    arrival = jnp.take_along_axis(earlier, residue, axis=2)
    group_id = grp_perm[dev_ids, residue]
    slot_pos = (exp_off[dev_ids, residue][..., None] + arrival[..., None] * PER_GROUP + jnp.arange(PER_GROUP)) % EXP_GROUP
    local_exp = jnp.take_along_axis(exp_perm[dev_ids, residue], slot_pos, axis=3)
    expert = group_id[..., None] * EXP_GROUP + local_exp
    routed = expert[jnp.arange(DEVS)[:, None], tok_order]
    return routed.reshape(ROWS, M_GROUPS, PER_GROUP).astype(jnp.int32)


def setup_inputs(seed: int = 0, part: int = 0) -> dict:
    base_key = jax.random.key(seed)
    part_key = jax.random.fold_in(base_key, part)
    key_tok, key_route, key_gate = jax.random.split(part_key, 3)
    key_one, key_three, key_two = jax.random.split(jax.random.key(seed + 1), 3)
    tokens = jax.random.normal(key_tok, (ROWS, D), jnp.float32).astype(jnp.bfloat16)
    expert_ids = draw_routing(key_route)
    gate_vals = jax.random.uniform(key_gate, (ROWS, M_GROUPS, PER_GROUP), jnp.float32, 0.3, 1.7) / TOP
    w_one = (jax.random.normal(key_one, (EXPERTS, D, FF), jnp.float32) * D ** -0.5).astype(jnp.bfloat16)
    w_three = (jax.random.normal(key_three, (EXPERTS, D, FF), jnp.float32) * D ** -0.5).astype(jnp.bfloat16)
    w_two = (jax.random.normal(key_two, (EXPERTS, FF, D), jnp.float32) * (2.0 * FF ** -0.5)).astype(jnp.bfloat16)
    return {'tokens': tokens, 'expert_ids': expert_ids, 'gate_vals': gate_vals, 'w_one': w_one, 'w_three': w_three, 'w_two': w_two}


def expert_rows(x_rows, w_first, w_third, w_second):
    h_one = jnp.dot(x_rows, w_first, preferred_element_type=jnp.float32)
    h_three = jnp.dot(x_rows, w_third, preferred_element_type=jnp.float32)
    act_bf = (jax.nn.silu(h_one) * h_three).astype(jnp.bfloat16)
    return jnp.dot(act_bf, w_second, preferred_element_type=jnp.float32).astype(jnp.bfloat16)


def reference(tokens, expert_ids, gate_vals, w_one, w_three, w_two):
    flat_ids = expert_ids.reshape(ROWS, TOP)
    flat_gate = gate_vals.reshape(ROWS, TOP)
    slot_ids = jnp.arange(EXP_ROWS)

    def one_expert(grp_acc, packed):
        exp_id, w_first, w_third, w_second = packed
        hit_mask = flat_ids == exp_id
        hit_any = jnp.any(hit_mask, axis=1)
        tok_gate = jnp.sum(jnp.where(hit_mask, flat_gate, 0.0), axis=1)
        row_ids = jnp.nonzero(hit_any, size=EXP_ROWS, fill_value=0)[0]
        row_gate = jnp.where(slot_ids < jnp.sum(hit_any.astype(jnp.int32)), tok_gate[row_ids], 0.0)
        exp_out = expert_rows(tokens[row_ids], w_first, w_third, w_second)
        grp_acc = grp_acc.at[row_ids].add(row_gate[:, None] * exp_out.astype(jnp.float32))
        return grp_acc, None

    def one_group(total_sum, packed):
        grp_acc, _ = lax.scan(one_expert, jnp.zeros((ROWS, D), jnp.float32), packed)
        return total_sum + grp_acc.astype(jnp.bfloat16).astype(jnp.float32), None

    packed_all = (jnp.arange(EXPERTS).reshape(GRP, EXP_GROUP), w_one.reshape(GRP, EXP_GROUP, D, FF), w_three.reshape(GRP, EXP_GROUP, D, FF), w_two.reshape(GRP, EXP_GROUP, FF, D))
    total_sum, _ = lax.scan(one_group, jnp.zeros((ROWS, D), jnp.float32), packed_all)
    return total_sum.astype(jnp.bfloat16)
```

```python
import functools

import jax
import jax.numpy as jnp
from jax import lax
from jax.experimental import pallas as pl
from jax.experimental.pallas import tpu as pltpu
from jax.sharding import PartitionSpec as P

BF = jnp.bfloat16
F32 = jnp.float32
MESH = pl.DeviceIdType.MESH
NC = 2
NT = (((1,), (1,)), ((), ()))


def dot(a, b):
    return jnp.dot(a, b, preferred_element_type=F32)


def dot_nt(a, b):
    return lax.dot_general(a, b, NT, preferred_element_type=F32)


def wait_bytes(ref, sem):
    pltpu.make_async_copy(ref, ref, sem).wait()


def moe_kernel(dims, tok_hbm, meta_ref, perm_ref, w1_hbm, w3_hbm, w2_hbm, y_ref,
               wa, wb, ag, ymeta, xmeta, sel, xin, act, actp, out, eb, gsum, grec,
               smat, cmat, fmat,
               wa_sem, wb_sem, tok_sem, meta_send, ymeta_recv, xmeta_recv,
               own_send, fwd_send, dn_recv, up_recv, far_recv,
               disp_send, disp_recv, comb_send, comb_recv, fin_send, fin_recv):
    (t_cnt, d_model, ff, nx, ny, e_loc, e_grp, cap_g, cap_e, top_k, cw) = dims
    nk = d_model // cw
    nd = nx * NC
    rows = nd * ny * cap_e
    grp = lax.axis_index('grp')
    j = lax.axis_index('ing')
    x = grp // NC
    c = grp % NC

    def at(dx, dc, dj):
        gx = lax.rem(x + dx, nx)
        cc = c if dc == 0 else (NC - 1) - c
        return gx * NC + cc, lax.rem(j + dj, ny)

    def dev(dx, dc, dj):
        gg, jj = at(dx, dc, dj)
        return {'grp': gg, 'ing': jj}

    def send(src, dst, ssem, rsem, where):
        pltpu.make_async_remote_copy(src_ref=src, dst_ref=dst, send_sem=ssem, recv_sem=rsem,
                                     device_id=dev(*where), device_id_type=MESH).start()

    def cols(k):
        return pl.ds(k * cw, cw)

    row_peers = [(dx, dc, 0) for dx in range(nx) for dc in range(NC) if dx or dc]
    col_peers = [(0, dc, dj) for dj in range(ny) for dc in range(NC) if dj or dc]
    far_first = sorted(row_peers, key=lambda p: -min(p[0], nx - p[0]))
    col_far_first = sorted(col_peers, key=lambda p: -min(p[2], ny - p[2]))

    tok_cp = pltpu.make_async_copy(tok_hbm, ag.at[0], tok_sem)
    tok_cp.start()
    wcopies = {}

    def load_w(name, src, dst, sem):
        cp = pltpu.make_async_copy(src, dst, sem)
        cp.start()
        wcopies[name] = cp

    load_w('1_0', w1_hbm.at[0], wa.at[0], wa_sem.at[0])
    load_w('3_0', w3_hbm.at[0], wa.at[1], wa_sem.at[1])
    load_w('2_0', w2_hbm.at[0], wb, wb_sem.at[0])
    load_w('1_1', w1_hbm.at[1], wa.at[2], wa_sem.at[2])

    barrier = pltpu.get_barrier_semaphore()
    peers = row_peers + [p for p in col_peers if p[2]]
    for p in peers:
        pl.semaphore_signal(barrier, inc=1, device_id=dev(*p), device_id_type=MESH)
    pl.semaphore_wait(barrier, len(peers))
    tok_cp.wait()

    for dj in range(1, ny):
        send(meta_ref, ymeta.at[ny - dj], meta_send.at[0], ymeta_recv, (0, 0, dj))
    for dx in range(1, nx):
        send(meta_ref, xmeta.at[nx - dx], meta_send.at[1], xmeta_recv, (dx, 0, 0))

    def send_own(k):
        send(ag.at[0, :, cols(k)], ag.at[ny - 1, :, cols(k)], own_send, dn_recv.at[k], (0, 0, 1))
        send(ag.at[0, :, cols(k)], ag.at[1, :, cols(k)], own_send, up_recv.at[k], (0, 0, ny - 1))

    def forward(k):
        half = t_cnt // 2
        wait_bytes(ag.at[ny - 1, :, cols(k)], dn_recv.at[k])
        src = ag.at[ny - 1, pl.ds(0, half), cols(k)]
        send(src, ag.at[2, pl.ds(0, half), cols(k)], fwd_send, far_recv.at[k], (0, 0, 1))
        wait_bytes(ag.at[1, :, cols(k)], up_recv.at[k])
        src = ag.at[1, pl.ds(half, half), cols(k)]
        send(src, ag.at[2, pl.ds(half, half), cols(k)], fwd_send, far_recv.at[k], (0, 0, ny - 1))

    send_own(0)
    send_own(1)

    upper = (lax.broadcasted_iota(jnp.int32, (t_cnt, t_cnt), 0)
             < lax.broadcasted_iota(jnp.int32, (t_cnt, t_cnt), 1)).astype(F32).astype(BF)

    def vec_of(scalars):
        r_io = lax.broadcasted_iota(jnp.int32, (len(scalars), t_cnt), 0)
        v = jnp.zeros((len(scalars), t_cnt), jnp.int32)
        for r, s in enumerate(scalars):
            v = jnp.where(r_io == r, s, v)
        return v.astype(F32)

    def chosen(meta, evec):
        hit = jnp.zeros(evec.shape, F32)
        for q in range(top_k):
            hit = jnp.where(meta[q:q + 1, :] == evec, 1.0, hit)
        return hit

    def one_hot(key, n):
        m = key.shape[0]
        io = lax.broadcasted_iota(jnp.int32, (m, n, t_cnt), 1).astype(F32)
        return key[:, None, :] == io

    e_disp = []
    for l in range(e_loc):
        for dx in range(nx):
            for dc in range(NC):
                gg, jj = at(dx, dc, 0)
                e_disp.append(gg * e_grp + jj * e_loc + l)
    e_disp = vec_of(e_disp)

    g_lo = vec_of([at(dx, dc, 0)[0] * e_grp for dx in range(nx) for dc in range(NC)])
    own = meta_ref[...]
    hit = jnp.zeros(g_lo.shape, F32)
    for q in range(top_k):
        row = own[q:q + 1, :]
        hit = jnp.where((row >= g_lo) & (row < g_lo + e_grp), 1.0, hit)
    key = jnp.where(hit > 0.0, dot(hit.astype(BF), upper), -1.0)
    ft = jnp.where(one_hot(key, cap_g), 1.0, 0.0).astype(BF).reshape(nd * cap_g, t_cnt)
    eye = (lax.broadcasted_iota(jnp.int32, (t_cnt, t_cnt), 0)
           == lax.broadcasted_iota(jnp.int32, (t_cnt, t_cnt), 1)).astype(F32).astype(BF)
    fmat[...] = dot_nt(eye, ft).astype(BF)

    ymeta[0] = own
    xmeta[0] = own
    wait_bytes(ymeta.at[pl.ds(1, ny - 1)], ymeta_recv)
    for s in range(ny):
        hit = chosen(ymeta[s], e_disp)
        key = jnp.where(hit > 0.0, dot(hit.astype(BF), upper) + s * cap_e, -1.0)
        for l in range(e_loc):
            oh = jnp.where(one_hot(key[l * nd:(l + 1) * nd], ny * cap_e), 1.0, 0.0)
            smat[l, :, s * t_cnt:(s + 1) * t_cnt] = oh.astype(BF).reshape(rows, t_cnt)

    def select(l, k):
        r = dot(smat[l], ag[:, :, cols(k)].reshape(ny * t_cnt, cw)).astype(BF)
        r = r.reshape(nd, ny * cap_e, cw)
        sel[l, :, :, cols(k)] = r
        xin[l, 0, :, cols(k)] = r[0]
        for dx, dc, _ in far_first:
            slot = ((nx - dx) % nx) * NC + dc
            send(sel.at[l, dx * NC + dc, :, cols(k)], xin.at[l, slot, :, cols(k)],
                 disp_send.at[l], disp_recv.at[l], (dx, dc, 0))

    for k in range(nk):
        forward(k)
        if k + 2 < nk:
            send_own(k + 2)
        if k >= 1:
            wait_bytes(ag.at[2, :, cols(k - 1)], far_recv.at[k - 1])
            select(0, k - 1)
    wait_bytes(ag.at[2, :, cols(nk - 1)], far_recv.at[nk - 1])
    select(0, nk - 1)
    for l in range(1, e_loc):
        for k in range(nk):
            select(l, k)

    wait_bytes(xmeta.at[pl.ds(1, nx - 1)], xmeta_recv)
    gates = 8
    for rg in range(NC):
        e_vec = []
        for dj in range(ny):
            for l in range(e_loc):
                gg, jj = at(0, rg, dj)
                e_vec.append(gg * e_grp + jj * e_loc + l)
        e_vec = vec_of(e_vec)
        gs_parts = []
        w_parts = [[], [], []]
        for s in range(nx):
            m = xmeta[s]
            hit = chosen(m, e_vec)
            gate = jnp.zeros(e_vec.shape, F32)
            for q in range(top_k):
                gate = jnp.where(m[q:q + 1, :] == e_vec, m[gates + q:gates + q + 1, :], gate)
            key = jnp.where(hit > 0.0, dot(hit.astype(BF), upper) + s * cap_e, -1.0)
            any_hit = jnp.max(hit, axis=0, keepdims=True)
            g_hit = jnp.broadcast_to(any_hit, hit.shape)
            g_rank = dot(g_hit.astype(BF), upper)[0:1, :]
            g_key = jnp.where(any_hit > 0.0, g_rank + s * cap_g, -1.0)
            g_io = lax.broadcasted_iota(jnp.int32, (nx * cap_g, t_cnt), 0).astype(F32)
            gs_parts.append(jnp.where(g_key == g_io, 1.0, 0.0).astype(BF))
            g1 = gate.astype(BF)
            rest = gate - g1.astype(F32)
            g2 = rest.astype(BF)
            g3 = (rest - g2.astype(F32)).astype(BF)
            oh = one_hot(key, nx * cap_e)
            for part, gp in zip(w_parts, (g1, g2, g3)):
                w = jnp.where(oh, gp.astype(F32)[:, None, :], 0.0)
                part.append(w.astype(BF).reshape(e_grp * nx * cap_e, t_cnt))
        gs = jnp.concatenate(gs_parts, axis=1)
        n_g = nx * cap_g
        for i in range(3):
            w = jnp.concatenate(w_parts[i], axis=1)
            cmat[rg, i * n_g:(i + 1) * n_g, :] = dot_nt(gs, w).astype(BF)

    nw = 256
    slots = {0: (0, 1), 1: (2, 0)}
    for l in range(e_loc):
        s1, s3 = slots[l]
        wait_bytes(xin.at[l, pl.ds(1, nd - 1)], disp_recv.at[l])
        wcopies['1_%d' % l].wait()
        wcopies['3_%d' % l].wait()

        def h_body(n, carry):
            cs = pl.ds(pl.multiple_of(n * nw, nw), nw)
            xr = xin[l].reshape(rows, d_model)
            h1 = dot(xr, wa[s1, :, cs])
            h3 = dot(xr, wa[s3, :, cs])
            act[:, cs] = (jax.nn.silu(h1) * h3).astype(BF)
            return carry

        lax.fori_loop(0, ff // nw, h_body, 0)
        if l == 0:
            load_w('3_1', w3_hbm.at[1], wa.at[0], wa_sem.at[0])

        def p_body(n, carry):
            cs = pl.ds(pl.multiple_of(n * cw, cw), cw)
            actp[:, cs] = dot(perm_ref[...], act[:, cs]).astype(BF)
            return carry

        lax.fori_loop(0, ff // cw, p_body, 0)
        wcopies['2_%d' % l].wait()
        for k in range(nk):
            o = dot(actp[...], wb[:, cols(k)]).astype(BF).reshape(NC * ny, nx * cap_e, cw)
            out[l, :, :, cols(k)] = o
            eb[0, l, :, cols(k)] = o[0]
            for _, dc, dj in col_far_first:
                slot = dc * ny + (ny - dj) % ny
                send(out.at[l, dc * ny + dj, :, cols(k)], eb.at[slot, l, :, cols(k)],
                     comb_send.at[l], comb_recv.at[l, k], (0, dc, dj))
        if l == 0:
            load_w('2_1', w2_hbm.at[1], wb, wb_sem.at[0])

    def merge(k):
        n_g = nx * cap_g
        for l in range(e_loc):
            wait_bytes(eb.at[pl.ds(1, NC * ny - 1), l, :, cols(k)], comb_recv.at[l, k])
        for rg in range(NC):
            e = eb[rg * ny:(rg + 1) * ny, :, :, cols(k)].reshape(ny * e_loc * nx * cap_e, cw)
            r = dot(cmat[rg], e)
            r = (r[0:n_g] + r[n_g:2 * n_g] + r[2 * n_g:3 * n_g]).astype(BF).reshape(nx, cap_g, cw)
            gsum[:, rg, :, cols(k)] = r
            grec[0, rg, :, cols(k)] = r[0]
        for dx in sorted(range(1, nx), key=lambda d: -min(d, nx - d)):
            send(gsum.at[dx, :, :, cols(k)], grec.at[nx - dx, :, :, cols(k)],
                 fin_send, fin_recv.at[k], (dx, 0, 0))

    def final(k):
        wait_bytes(grec.at[pl.ds(1, nx - 1), :, :, cols(k)], fin_recv.at[k])
        g = grec[:, :, :, cols(k)].reshape(nd * cap_g, cw)
        y_ref[:, cols(k)] = dot(fmat[...], g).astype(BF)

    for k in range(nk):
        merge(k)
        if k >= 1:
            final(k - 1)
    final(nk - 1)

    wait_bytes(ymeta.at[pl.ds(1, ny - 1)], meta_send.at[0])
    wait_bytes(xmeta.at[pl.ds(1, nx - 1)], meta_send.at[1])
    wait_bytes(ag.at[pl.ds(0, 2)], own_send)
    wait_bytes(ag.at[0], fwd_send)
    for l in range(e_loc):
        wait_bytes(sel.at[l, pl.ds(1, nd - 1)], disp_send.at[l])
        wait_bytes(out.at[l, pl.ds(1, NC * ny - 1)], comb_send.at[l])
    wait_bytes(gsum.at[pl.ds(1, nx - 1)], fin_send)


def solution(mesh):
    n_grp = mesh.shape['grp']
    ny = mesh.shape['ing']
    nx = n_grp // NC
    row_spec = P(('dp', 'grp', 'ing'))
    exp_spec = P(('grp', 'ing'))

    def local_fn(tokens, expert_ids, gate_vals, w_one, w_three, w_two):
        t_cnt, d_model = tokens.shape
        m_groups, per_group = expert_ids.shape[1:]
        top_k = m_groups * per_group
        e_loc, _, ff = w_one.shape
        e_grp = e_loc * ny
        cap_g = (t_cnt * m_groups + n_grp - 1) // n_grp
        cap_e = (cap_g * per_group + e_grp - 1) // e_grp
        cw = 512
        nk = d_model // cw
        rows = n_grp * ny * cap_e
        dims = (t_cnt, d_model, ff, nx, ny, e_loc, e_grp, cap_g, cap_e, top_k, cw)

        ids_t = expert_ids.reshape(t_cnt, top_k).astype(F32).T
        gate_t = gate_vals.reshape(t_cnt, top_k).T
        pad = ((0, 8 - top_k), (0, 0))
        meta = jnp.concatenate([jnp.pad(ids_t, pad, constant_values=-1.0), jnp.pad(gate_t, pad)], axis=0)

        o = lax.broadcasted_iota(jnp.int32, (rows, rows), 0)
        i = lax.broadcasted_iota(jnp.int32, (rows, rows), 1)
        blk_o, q = o // cap_e, o % cap_e
        rx, rest = blk_o % nx, blk_o // nx
        rj, rc = rest % ny, rest // ny
        perm = (i == ((rx * NC + rc) * ny + rj) * cap_e + q).astype(BF)

        vm, dma = pltpu.VMEM, pltpu.SemaphoreType.DMA
        hbm = pl.BlockSpec(memory_space=pltpu.HBM)
        vmem = pl.BlockSpec(memory_space=pltpu.VMEM)
        blk = nx * cap_e
        return pl.pallas_call(
            functools.partial(moe_kernel, dims),
            out_shape=jax.ShapeDtypeStruct((t_cnt, d_model), BF),
            in_specs=[hbm, vmem, vmem, hbm, hbm, hbm],
            out_specs=vmem,
            scratch_shapes=[
                vm((3, d_model, ff), BF), vm((ff, d_model), BF),
                vm((ny, t_cnt, d_model), BF), vm((ny, 16, t_cnt), F32), vm((nx, 16, t_cnt), F32),
                vm((e_loc, n_grp, ny * cap_e, d_model), BF), vm((e_loc, n_grp, ny * cap_e, d_model), BF),
                vm((rows, ff), BF), vm((rows, ff), BF),
                vm((e_loc, NC * ny, blk, d_model), BF), vm((NC * ny, e_loc, blk, d_model), BF),
                vm((nx, NC, cap_g, d_model), BF), vm((nx, NC, cap_g, d_model), BF),
                vm((e_loc, rows, ny * t_cnt), BF), vm((NC, 3 * nx * cap_g, e_grp * blk), BF),
                vm((t_cnt, n_grp * cap_g), BF),
                dma((3,)), dma((1,)), dma, dma((2,)), dma, dma,
                dma, dma, dma((nk,)), dma((nk,)), dma((nk,)),
                dma((e_loc,)), dma((e_loc,)), dma((e_loc,)), dma((e_loc, nk)), dma, dma((nk,)),
            ],
            compiler_params=pltpu.CompilerParams(
                collective_id=0, has_side_effects=True, vmem_limit_bytes=67043328),
        )(tokens, meta, perm, w_one, w_three, w_two)

    return jax.shard_map(local_fn, mesh=mesh, in_specs=(row_spec, row_spec, row_spec, exp_spec, exp_spec, exp_spec), out_specs=row_spec, check_vma=False)
```

```python
import functools

import jax
import jax.numpy as jnp
from jax import lax
from jax.experimental import pallas as pl
from jax.experimental.pallas import tpu as pltpu
from jax.sharding import PartitionSpec as P

BF = jnp.bfloat16
F32 = jnp.float32
MESH = pl.DeviceIdType.MESH
NC = 2
NT = (((1,), (1,)), ((), ()))


def dot(a, b):
    return jnp.dot(a, b, preferred_element_type=F32)


def dot_nt(a, b):
    return lax.dot_general(a, b, NT, preferred_element_type=F32)


def wait_bytes(ref, sem):
    pltpu.make_async_copy(ref, ref, sem).wait()


def moe_kernel(dims, tok_hbm, ids_ref, gates_ref, w1_hbm, w3_hbm, w2_hbm, y_ref,
               wa, wb, ag, yids, xids, xgates, sel, xin, xp, h1, h3, act, out, eb, gsum, grec,
               perm, smat, cmat, fmat,
               wa_sem, wb_sem, tok_sem, meta_send, meta_recv,
               own_send, fwd_send, dn_recv, up_recv, far_recv,
               disp_send, disp_recv, comb_send, comb_recv, fin_send, fin_recv):
    (t_cnt, d_model, ff, nx, ny, e_loc, e_grp, cap_g, cap_e, cw) = dims
    m_groups, per_group, _ = ids_ref.shape
    picks = [(m, u) for m in range(m_groups) for u in range(per_group)]
    nk = d_model // cw
    nd = nx * NC
    rows = nd * ny * cap_e
    grp = lax.axis_index('grp')
    j = lax.axis_index('ing')
    x = grp // NC
    c = grp % NC

    def at(dx, dc, dj):
        gx = lax.rem(x + dx, nx)
        cc = c if dc == 0 else (NC - 1) - c
        return gx * NC + cc, lax.rem(j + dj, ny)

    def dev(dx, dc, dj):
        gg, jj = at(dx, dc, dj)
        return {'grp': gg, 'ing': jj}

    def send(src, dst, ssem, rsem, where):
        pltpu.make_async_remote_copy(src_ref=src, dst_ref=dst, send_sem=ssem, recv_sem=rsem,
                                     device_id=dev(*where), device_id_type=MESH).start()

    def cols(k):
        return pl.ds(k * cw, cw)

    row_peers = [(dx, dc, 0) for dx in range(nx) for dc in range(NC) if dx or dc]
    col_peers = [(0, dc, dj) for dj in range(ny) for dc in range(NC) if dj or dc]
    far_first = sorted(row_peers, key=lambda p: -min(p[0], nx - p[0]))
    col_far_first = sorted(col_peers, key=lambda p: -min(p[2], ny - p[2]))

    tok_cp = pltpu.make_async_copy(tok_hbm, ag.at[0], tok_sem)
    tok_cp.start()
    wcopies = {}

    def load_w(name, src, dst, sem):
        cp = pltpu.make_async_copy(src, dst, sem)
        cp.start()
        wcopies[name] = cp

    barrier = pltpu.get_barrier_semaphore()
    peers = row_peers + [p for p in col_peers if p[2]]
    for p in peers:
        pl.semaphore_signal(barrier, inc=1, device_id=dev(*p), device_id_type=MESH)
    with jax.named_scope('barrier_wait'):
        pl.semaphore_wait(barrier, len(peers))
        tok_cp.wait()

    for dj in range(1, ny):
        send(ids_ref, yids.at[ny - dj], meta_send.at[0], meta_recv.at[0], (0, 0, dj))
    for dx in range(1, nx):
        send(ids_ref, xids.at[nx - dx], meta_send.at[1], meta_recv.at[1], (dx, 0, 0))
        send(gates_ref, xgates.at[nx - dx], meta_send.at[2], meta_recv.at[2], (dx, 0, 0))

    def send_own(k):
        send(ag.at[0, :, cols(k)], ag.at[ny - 1, :, cols(k)], own_send, dn_recv.at[k], (0, 0, 1))
        send(ag.at[0, :, cols(k)], ag.at[1, :, cols(k)], own_send, up_recv.at[k], (0, 0, ny - 1))

    def forward(k):
        half = t_cnt // 2
        with jax.named_scope('wait_dn#k=%d' % k):
            wait_bytes(ag.at[ny - 1, :, cols(k)], dn_recv.at[k])
        src = ag.at[ny - 1, pl.ds(0, half), cols(k)]
        send(src, ag.at[2, pl.ds(0, half), cols(k)], fwd_send, far_recv.at[k], (0, 0, 1))
        with jax.named_scope('wait_up#k=%d' % k):
            wait_bytes(ag.at[1, :, cols(k)], up_recv.at[k])
        src = ag.at[1, pl.ds(half, half), cols(k)]
        send(src, ag.at[2, pl.ds(half, half), cols(k)], fwd_send, far_recv.at[k], (0, 0, ny - 1))

    send_own(0)
    send_own(1)

    upper = (lax.broadcasted_iota(jnp.int32, (t_cnt, t_cnt), 0)
             < lax.broadcasted_iota(jnp.int32, (t_cnt, t_cnt), 1)).astype(F32).astype(BF)

    def vec_of(scalars):
        r_io = lax.broadcasted_iota(jnp.int32, (len(scalars), t_cnt), 0)
        v = jnp.zeros((len(scalars), t_cnt), jnp.int32)
        for r, s in enumerate(scalars):
            v = jnp.where(r_io == r, s, v)
        return v

    def chosen(ids, s, evec):
        hit = jnp.zeros(evec.shape, F32)
        for m, u in picks:
            hit = jnp.where(ids[s, m, u:u + 1, :] == evec, 1.0, hit)
        return hit

    def one_hot(key, n):
        m = key.shape[0]
        io = lax.broadcasted_iota(jnp.int32, (m, n, t_cnt), 1).astype(F32)
        return key[:, None, :] == io

    e_disp = []
    for l in range(e_loc):
        for dx in range(nx):
            for dc in range(NC):
                gg, jj = at(dx, dc, 0)
                e_disp.append(gg * e_grp + jj * e_loc + l)
    e_disp = vec_of(e_disp)

    g_lo = vec_of([at(dx, dc, 0)[0] * e_grp for dx in range(nx) for dc in range(NC)])
    hit = jnp.zeros(g_lo.shape, F32)
    for m, u in picks:
        row = ids_ref[m, u:u + 1, :]
        hit = jnp.where((row >= g_lo) & (row < g_lo + e_grp), 1.0, hit)
    key = jnp.where(hit > 0.0, dot(hit.astype(BF), upper), -1.0)
    ft = jnp.where(one_hot(key, cap_g), 1.0, 0.0).astype(BF).reshape(nd * cap_g, t_cnt)
    eye = (lax.broadcasted_iota(jnp.int32, (t_cnt, t_cnt), 0)
           == lax.broadcasted_iota(jnp.int32, (t_cnt, t_cnt), 1)).astype(F32).astype(BF)
    fmat[...] = dot_nt(eye, ft).astype(BF)

    yids[0] = ids_ref[...]
    xids[0] = ids_ref[...]
    xgates[0] = gates_ref[...]

    def split(v, n):
        hi = jnp.floor((v + 0.5) * (1.0 / n))
        return hi, v - hi * n

    blk_o, q_o = split(lax.broadcasted_iota(jnp.int32, (rows, rows), 0).astype(F32), cap_e)
    rest_o, rx_o = split(blk_o, nx)
    rc_o, rj_o = split(rest_o, ny)
    src = ((rx_o * NC + rc_o) * ny + rj_o) * cap_e + q_o
    src_io = lax.broadcasted_iota(jnp.int32, (rows, rows), 1).astype(F32)
    perm[...] = jnp.where(src == src_io, 1.0, 0.0).astype(BF)

    with jax.named_scope('wait_yids'):
        wait_bytes(yids.at[pl.ds(1, ny - 1)], meta_recv.at[0])
    load_w('1_0', w1_hbm.at[0], wa.at[0], wa_sem.at[0])
    load_w('3_0', w3_hbm.at[0], wa.at[1], wa_sem.at[1])
    for s in range(ny):
        hit = chosen(yids, s, e_disp)
        key = jnp.where(hit > 0.0, dot(hit.astype(BF), upper) + s * cap_e, -1.0)
        for l in range(e_loc):
            oh = jnp.where(one_hot(key[l * nd:(l + 1) * nd], ny * cap_e), 1.0, 0.0)
            smat[l, :, s * t_cnt:(s + 1) * t_cnt] = oh.astype(BF).reshape(rows, t_cnt)

    def select(l, k):
        r = dot(smat[l], ag[:, :, cols(k)].reshape(ny * t_cnt, cw)).astype(BF)
        r = r.reshape(nd, ny * cap_e, cw)
        sel[l, :, :, cols(k)] = r
        xin[l, 0, :, cols(k)] = r[0]
        for dx, dc, _ in far_first:
            slot = ((nx - dx) % nx) * NC + dc
            send(sel.at[l, dx * NC + dc, :, cols(k)], xin.at[l, slot, :, cols(k)],
                 disp_send.at[l], disp_recv.at[l, k], (dx, dc, 0))

    for k in range(nk):
        forward(k)
        if k + 2 < nk:
            send_own(k + 2)
        if k >= 1:
            with jax.named_scope('wait_far#k=%d' % (k - 1)):
                wait_bytes(ag.at[2, :, cols(k - 1)], far_recv.at[k - 1])
            with jax.named_scope('select0#k=%d' % (k - 1)):
                select(0, k - 1)
    with jax.named_scope('wait_far#k=%d' % (nk - 1)):
        wait_bytes(ag.at[2, :, cols(nk - 1)], far_recv.at[nk - 1])
    with jax.named_scope('select0#k=%d' % (nk - 1)):
        select(0, nk - 1)
    for l in range(1, e_loc):
        for k in range(nk):
            with jax.named_scope('select1#k=%d' % k):
                select(l, k)

    load_w('2_0', w2_hbm.at[0], wb, wb_sem.at[0])
    load_w('1_1', w1_hbm.at[1], wa.at[2], wa_sem.at[2])
    with jax.named_scope('wait_xids'):
        wait_bytes(xids.at[pl.ds(1, nx - 1)], meta_recv.at[1])
        wait_bytes(xgates.at[pl.ds(1, nx - 1)], meta_recv.at[2])
    for rg in range(NC):
        e_vec = []
        for dj in range(ny):
            for l in range(e_loc):
                gg, jj = at(0, rg, dj)
                e_vec.append(gg * e_grp + jj * e_loc + l)
        e_vec = vec_of(e_vec)
        gs_parts = []
        w_parts = [[], [], []]
        for s in range(nx):
            hit = chosen(xids, s, e_vec)
            gate = jnp.zeros(e_vec.shape, F32)
            for m, u in picks:
                gate = jnp.where(xids[s, m, u:u + 1, :] == e_vec, xgates[s, m, u:u + 1, :], gate)
            key = jnp.where(hit > 0.0, dot(hit.astype(BF), upper) + s * cap_e, -1.0)
            any_hit = jnp.max(hit, axis=0, keepdims=True)
            g_hit = jnp.broadcast_to(any_hit, hit.shape)
            g_rank = dot(g_hit.astype(BF), upper)[0:1, :]
            g_key = jnp.where(any_hit > 0.0, g_rank + s * cap_g, -1.0)
            g_io = lax.broadcasted_iota(jnp.int32, (nx * cap_g, t_cnt), 0).astype(F32)
            gs_parts.append(jnp.where(g_key == g_io, 1.0, 0.0).astype(BF))
            g1 = gate.astype(BF)
            rest = gate - g1.astype(F32)
            g2 = rest.astype(BF)
            g3 = (rest - g2.astype(F32)).astype(BF)
            oh = one_hot(key, nx * cap_e)
            for part, gp in zip(w_parts, (g1, g2, g3)):
                w = jnp.where(oh, gp.astype(F32)[:, None, :], 0.0)
                part.append(w.astype(BF).reshape(e_grp * nx * cap_e, t_cnt))
        gs = jnp.concatenate(gs_parts, axis=1)
        n_g = nx * cap_g
        for i in range(3):
            w = jnp.concatenate(w_parts[i], axis=1)
            cmat[rg, i * n_g:(i + 1) * n_g, :] = dot_nt(gs, w).astype(BF)

    nw = ff // 2
    slots = {0: (0, 1), 1: (2, 0)}

    def up_proj(l, k):
        s1, s3 = slots[l]
        with jax.named_scope('wait_rows#l=%d,k=%d' % (l, k)):
            wait_bytes(xin.at[l, pl.ds(1, nd - 1), :, cols(k)], disp_recv.at[l, k])
        if k == 0:
            with jax.named_scope('wait_w13#l=%d' % l):
                wcopies['1_%d' % l].wait()
                wcopies['3_%d' % l].wait()
        with jax.named_scope('perm#l=%d,k=%d' % (l, k)):
            xp[...] = dot(perm[...], xin[l, :, :, cols(k)].reshape(rows, cw)).astype(BF)

        def body(n, carry):
            cs = pl.ds(pl.multiple_of(n * nw, nw), nw)
            d1 = dot(xp[...], wa[s1, cols(k), cs])
            d3 = dot(xp[...], wa[s3, cols(k), cs])
            if k:
                d1 = d1 + h1[:, cs]
                d3 = d3 + h3[:, cs]
            if k < nk - 1:
                h1[:, cs] = d1
                h3[:, cs] = d3
            else:
                act[:, cs] = (jax.nn.silu(d1) * d3).astype(BF)
            return carry

        with jax.named_scope('h#l=%d,k=%d' % (l, k)):
            lax.fori_loop(0, ff // nw, body, 0)

    for l in range(e_loc):
        for k in range(nk):
            up_proj(l, k)
        if l == 0:
            load_w('3_1', w3_hbm.at[1], wa.at[0], wa_sem.at[0])
        with jax.named_scope('wait_w2#l=%d' % l):
            wcopies['2_%d' % l].wait()
        for k in range(nk):
            with jax.named_scope('w2#l=%d' % l):
                o = dot(act[...], wb[:, cols(k)]).astype(BF).reshape(NC * ny, nx * cap_e, cw)
                out[l, :, :, cols(k)] = o
                eb[0, l, :, cols(k)] = o[0]
            for _, dc, dj in col_far_first:
                slot = dc * ny + (ny - dj) % ny
                send(out.at[l, dc * ny + dj, :, cols(k)], eb.at[slot, l, :, cols(k)],
                     comb_send.at[l], comb_recv.at[l, k], (0, dc, dj))
        if l == 0:
            load_w('2_1', w2_hbm.at[1], wb, wb_sem.at[0])

    def merge(k):
        n_g = nx * cap_g
        for l in range(e_loc):
            with jax.named_scope('wait_comb#l=%d,k=%d' % (l, k)):
                wait_bytes(eb.at[pl.ds(1, NC * ny - 1), l, :, cols(k)], comb_recv.at[l, k])
        for rg in range(NC):
            e = eb[rg * ny:(rg + 1) * ny, :, :, cols(k)].reshape(ny * e_loc * nx * cap_e, cw)
            r = dot(cmat[rg], e)
            r = (r[0:n_g] + r[n_g:2 * n_g] + r[2 * n_g:3 * n_g]).astype(BF).reshape(nx, cap_g, cw)
            gsum[:, rg, :, cols(k)] = r
            grec[0, rg, :, cols(k)] = r[0]
        for dx in sorted(range(1, nx), key=lambda d: -min(d, nx - d)):
            send(gsum.at[dx, :, :, cols(k)], grec.at[nx - dx, :, :, cols(k)],
                 fin_send, fin_recv.at[k], (dx, 0, 0))

    def final(k):
        with jax.named_scope('wait_fin#k=%d' % k):
            wait_bytes(grec.at[pl.ds(1, nx - 1), :, :, cols(k)], fin_recv.at[k])
        g = grec[:, :, :, cols(k)].reshape(nd * cap_g, cw)
        y_ref[:, cols(k)] = dot(fmat[...], g).astype(BF)

    for k in range(nk):
        merge(k)
        if k >= 1:
            final(k - 1)
    final(nk - 1)

    wait_bytes(yids.at[pl.ds(1, ny - 1)], meta_send.at[0])
    wait_bytes(xids.at[pl.ds(1, nx - 1)], meta_send.at[1])
    wait_bytes(xgates.at[pl.ds(1, nx - 1)], meta_send.at[2])
    wait_bytes(ag.at[pl.ds(0, 2)], own_send)
    wait_bytes(ag.at[0], fwd_send)
    for l in range(e_loc):
        wait_bytes(sel.at[l, pl.ds(1, nd - 1)], disp_send.at[l])
        wait_bytes(out.at[l, pl.ds(1, NC * ny - 1)], comb_send.at[l])
    wait_bytes(gsum.at[pl.ds(1, nx - 1)], fin_send)


def solution(mesh):
    n_grp = mesh.shape['grp']
    ny = mesh.shape['ing']
    nx = n_grp // NC
    row_spec = P(('dp', 'grp', 'ing'))
    exp_spec = P(('grp', 'ing'))

    def local_fn(tokens, expert_ids, gate_vals, w_one, w_three, w_two):
        t_cnt, d_model = tokens.shape
        m_groups, per_group = expert_ids.shape[1:]
        e_loc, _, ff = w_one.shape
        e_grp = e_loc * ny
        cap_g = (t_cnt * m_groups + n_grp - 1) // n_grp
        cap_e = (cap_g * per_group + e_grp - 1) // e_grp
        cw = 512
        nk = d_model // cw
        rows = n_grp * ny * cap_e
        dims = (t_cnt, d_model, ff, nx, ny, e_loc, e_grp, cap_g, cap_e, cw)

        ids_t = jnp.transpose(expert_ids, (1, 2, 0))
        gate_t = jnp.transpose(gate_vals, (1, 2, 0))

        vm, dma = pltpu.VMEM, pltpu.SemaphoreType.DMA
        hbm = pl.BlockSpec(memory_space=pltpu.HBM)
        vmem = pl.BlockSpec(memory_space=pltpu.VMEM)
        blk = nx * cap_e
        return pl.pallas_call(
            functools.partial(moe_kernel, dims),
            out_shape=jax.ShapeDtypeStruct((t_cnt, d_model), BF),
            in_specs=[hbm, vmem, vmem, hbm, hbm, hbm],
            out_specs=vmem,
            scratch_shapes=[
                vm((3, d_model, ff), BF), vm((ff, d_model), BF),
                vm((ny, t_cnt, d_model), BF),
                vm((ny,) + ids_t.shape, jnp.int32), vm((nx,) + ids_t.shape, jnp.int32), vm((nx,) + ids_t.shape, F32),
                vm((e_loc, n_grp, ny * cap_e, d_model), BF), vm((e_loc, n_grp, ny * cap_e, d_model), BF),
                vm((rows, cw), BF), vm((rows, ff), F32), vm((rows, ff), F32), vm((rows, ff), BF),
                vm((e_loc, NC * ny, blk, d_model), BF), vm((NC * ny, e_loc, blk, d_model), BF),
                vm((nx, NC, cap_g, d_model), BF), vm((nx, NC, cap_g, d_model), BF),
                vm((rows, rows), BF), vm((e_loc, rows, ny * t_cnt), BF), vm((NC, 3 * nx * cap_g, e_grp * blk), BF),
                vm((t_cnt, n_grp * cap_g), BF),
                dma((3,)), dma((1,)), dma, dma((3,)), dma((3,)),
                dma, dma, dma((nk,)), dma((nk,)), dma((nk,)),
                dma((e_loc,)), dma((e_loc, nk)), dma((e_loc,)), dma((e_loc, nk)), dma, dma((nk,)),
            ],
            compiler_params=pltpu.CompilerParams(
                collective_id=0, has_side_effects=True, vmem_limit_bytes=67043328),
        )(tokens, ids_t, gate_t, w_one, w_three, w_two)

    return jax.shard_map(local_fn, mesh=mesh, in_specs=(row_spec, row_spec, row_spec, exp_spec, exp_spec, exp_spec), out_specs=row_spec, check_vma=False)
```

```python
import functools

import jax
import jax.numpy as jnp
from jax import lax
from jax.experimental import pallas as pl
from jax.experimental.pallas import tpu as pltpu
from jax.sharding import PartitionSpec as P

BF = jnp.bfloat16
F32 = jnp.float32
MESH = pl.DeviceIdType.MESH
NC = 2
NT = (((1,), (1,)), ((), ()))


def dot(a, b):
    return jnp.dot(a, b, preferred_element_type=F32)


def dot_nt(a, b):
    return lax.dot_general(a, b, NT, preferred_element_type=F32)


def wait_bytes(ref, sem):
    pltpu.make_async_copy(ref, ref, sem).wait()


def moe_kernel(dims, tok_hbm, ids_ref, gates_ref, w1_hbm, w3_hbm, w2_hbm, y_ref,
               wa, wb, ag, xag, yids, xids, xgates, sel, sela, xin, xa, xp, h1, h3, act, out, eb,
               gsum, grec, perm, smat, smata, cmat, fmat,
               wa_sem, wb_sem, tok_sem, meta_send, meta_recv,
               own_send, fwd_send, dn_recv, up_recv, far_recv,
               xag_send, xag_recv, disp_send, dispa_send, disp_recv, comb_send, comb_recv, fin_send, fin_recv):
    (t_cnt, d_model, ff, nx, ny, e_loc, e_grp, cap_g, cap_e, cw, aw, nw2) = dims
    m_groups, per_group, _ = ids_ref.shape
    picks = [(m, u) for m in range(m_groups) for u in range(per_group)]
    bw = d_model - aw
    nk = bw // cw
    nd = nx * NC
    rows = nd * ny * cap_e
    grp = lax.axis_index('grp')
    j = lax.axis_index('ing')
    x = grp // NC
    c = grp % NC

    def at(dx, dc, dj):
        gx = lax.rem(x + dx, nx)
        cc = c if dc == 0 else (NC - 1) - c
        return gx * NC + cc, lax.rem(j + dj, ny)

    def dev(dx, dc, dj):
        gg, jj = at(dx, dc, dj)
        return {'grp': gg, 'ing': jj}

    def send(src, dst, ssem, rsem, where):
        pltpu.make_async_remote_copy(src_ref=src, dst_ref=dst, send_sem=ssem, recv_sem=rsem,
                                     device_id=dev(*where), device_id_type=MESH).start()

    def cols(k):
        return pl.ds(k * cw, cw)

    row_peers = [(dx, dc, 0) for dx in range(nx) for dc in range(NC) if dx or dc]
    col_peers = [(0, dc, dj) for dj in range(ny) for dc in range(NC) if dj or dc]
    far_first = sorted(row_peers, key=lambda p: -min(p[0], nx - p[0]))
    col_far_first = sorted(col_peers, key=lambda p: -min(p[2], ny - p[2]))

    tok_cp = pltpu.make_async_copy(tok_hbm.at[:, pl.ds(0, bw)], ag.at[0], tok_sem.at[0])
    tok_cp.start()
    toka_cp = pltpu.make_async_copy(tok_hbm.at[:, pl.ds(bw, aw)], xag.at[0], tok_sem.at[1])
    toka_cp.start()
    wcopies = {}

    def load_w(name, src, dst, sem):
        cp = pltpu.make_async_copy(src, dst, sem)
        cp.start()
        wcopies[name] = cp

    barrier = pltpu.get_barrier_semaphore()
    peers = row_peers + [p for p in col_peers if p[2]]
    for p in peers:
        pl.semaphore_signal(barrier, inc=1, device_id=dev(*p), device_id_type=MESH)
    with jax.named_scope('barrier_wait'):
        pl.semaphore_wait(barrier, len(peers))
        tok_cp.wait()
        toka_cp.wait()

    for dj in range(1, ny):
        send(ids_ref, yids.at[ny - dj], meta_send.at[0], meta_recv.at[0], (0, 0, dj))
    for dx in range(1, nx):
        send(ids_ref, xids.at[nx - dx], meta_send.at[1], meta_recv.at[1], (dx, 0, 0))
        send(gates_ref, xgates.at[nx - dx], meta_send.at[2], meta_recv.at[2], (dx, 0, 0))

    def send_own(k):
        send(ag.at[0, :, cols(k)], ag.at[ny - 1, :, cols(k)], own_send, dn_recv.at[k], (0, 0, 1))
        send(ag.at[0, :, cols(k)], ag.at[1, :, cols(k)], own_send, up_recv.at[k], (0, 0, ny - 1))

    def forward(k):
        half = t_cnt // 2
        with jax.named_scope('wait_dn#k=%d' % k):
            wait_bytes(ag.at[ny - 1, :, cols(k)], dn_recv.at[k])
        src = ag.at[ny - 1, pl.ds(0, half), cols(k)]
        send(src, ag.at[2, pl.ds(0, half), cols(k)], fwd_send, far_recv.at[k], (0, 0, 1))
        with jax.named_scope('wait_up#k=%d' % k):
            wait_bytes(ag.at[1, :, cols(k)], up_recv.at[k])
        src = ag.at[1, pl.ds(half, half), cols(k)]
        send(src, ag.at[2, pl.ds(half, half), cols(k)], fwd_send, far_recv.at[k], (0, 0, ny - 1))

    ahead = 3
    for k in range(ahead):
        send_own(k)
    half = t_cnt // 2
    send(xag.at[0], xag.at[nx - 1], xag_send.at[0], xag_recv.at[0], (1, 0, 0))
    send(xag.at[0], xag.at[1], xag_send.at[0], xag_recv.at[1], (nx - 1, 0, 0))

    def x_forward():
        wait_bytes(xag.at[nx - 1], xag_recv.at[0])
        send(xag.at[nx - 1, pl.ds(0, half)], xag.at[2, pl.ds(0, half)], xag_send.at[1], xag_recv.at[2], (1, 0, 0))
        wait_bytes(xag.at[1], xag_recv.at[1])
        send(xag.at[1, pl.ds(half, half)], xag.at[2, pl.ds(half, half)], xag_send.at[1], xag_recv.at[2],
             (nx - 1, 0, 0))

    upper = (lax.broadcasted_iota(jnp.int32, (t_cnt, t_cnt), 0)
             < lax.broadcasted_iota(jnp.int32, (t_cnt, t_cnt), 1)).astype(F32).astype(BF)

    def vec_of(scalars):
        r_io = lax.broadcasted_iota(jnp.int32, (len(scalars), t_cnt), 0)
        v = jnp.zeros((len(scalars), t_cnt), jnp.int32)
        for r, s in enumerate(scalars):
            v = jnp.where(r_io == r, s, v)
        return v

    def chosen(ids, s, evec):
        hit = jnp.zeros(evec.shape, F32)
        for m, u in picks:
            hit = jnp.where(ids[s, m, u:u + 1, :] == evec, 1.0, hit)
        return hit

    def one_hot(key, n):
        m = key.shape[0]
        io = lax.broadcasted_iota(jnp.int32, (m, n, t_cnt), 1).astype(F32)
        return key[:, None, :] == io

    e_disp = []
    for l in range(e_loc):
        for dx in range(nx):
            for dc in range(NC):
                gg, jj = at(dx, dc, 0)
                e_disp.append(gg * e_grp + jj * e_loc + l)
    e_disp = vec_of(e_disp)

    g_lo = vec_of([at(dx, dc, 0)[0] * e_grp for dx in range(nx) for dc in range(NC)])
    hit = jnp.zeros(g_lo.shape, F32)
    for m, u in picks:
        row = ids_ref[m, u:u + 1, :]
        hit = jnp.where((row >= g_lo) & (row < g_lo + e_grp), 1.0, hit)
    key = jnp.where(hit > 0.0, dot(hit.astype(BF), upper), -1.0)
    ft = jnp.where(one_hot(key, cap_g), 1.0, 0.0).astype(BF).reshape(nd * cap_g, t_cnt)
    eye = (lax.broadcasted_iota(jnp.int32, (t_cnt, t_cnt), 0)
           == lax.broadcasted_iota(jnp.int32, (t_cnt, t_cnt), 1)).astype(F32).astype(BF)
    fmat[...] = dot_nt(eye, ft).astype(BF)

    yids[0] = ids_ref[...]
    xids[0] = ids_ref[...]
    xgates[0] = gates_ref[...]

    def split(v, n):
        hi = jnp.floor((v + 0.5) * (1.0 / n))
        return hi, v - hi * n

    blk_o, q_o = split(lax.broadcasted_iota(jnp.int32, (rows, rows), 0).astype(F32), cap_e)
    rest_o, rx_o = split(blk_o, nx)
    rc_o, rj_o = split(rest_o, ny)
    src = ((rx_o * NC + rc_o) * ny + rj_o) * cap_e + q_o
    src_io = lax.broadcasted_iota(jnp.int32, (rows, rows), 1).astype(F32)
    perm[...] = jnp.where(src == src_io, 1.0, 0.0).astype(BF)

    with jax.named_scope('wait_yids'):
        wait_bytes(yids.at[pl.ds(1, ny - 1)], meta_recv.at[0])
    load_w('1_0', w1_hbm.at[0], wa.at[0], wa_sem.at[0])
    load_w('3_0', w3_hbm.at[0], wa.at[1], wa_sem.at[1])
    for s in range(ny):
        hit = chosen(yids, s, e_disp)
        key = jnp.where(hit > 0.0, dot(hit.astype(BF), upper) + s * cap_e, -1.0)
        for l in range(e_loc):
            oh = jnp.where(one_hot(key[l * nd:(l + 1) * nd], ny * cap_e), 1.0, 0.0)
            smat[l, :, s * t_cnt:(s + 1) * t_cnt] = oh.astype(BF).reshape(rows, t_cnt)

    col_vecs = []
    for rg in range(NC):
        e_vec = []
        for dj in range(ny):
            for l in range(e_loc):
                gg, jj = at(0, rg, dj)
                e_vec.append(gg * e_grp + jj * e_loc + l)
        col_vecs.append(vec_of(e_vec))

    def col_key(rg, s):
        hit = chosen(xids, s, col_vecs[rg])
        return hit, jnp.where(hit > 0.0, dot(hit.astype(BF), upper) + s * cap_e, -1.0)

    with jax.named_scope('wait_xids'):
        wait_bytes(xids.at[pl.ds(1, nx - 1)], meta_recv.at[1])
    for s in range(nx):
        keys = [col_key(rg, s)[1] for rg in range(NC)]
        for l in range(e_loc):
            key = jnp.concatenate([keys[rg][dj * e_loc + l:dj * e_loc + l + 1]
                                   for rg in range(NC) for dj in range(ny)], axis=0)
            oh = jnp.where(one_hot(key, nx * cap_e), 1.0, 0.0)
            smata[l, :, s * t_cnt:(s + 1) * t_cnt] = oh.astype(BF).reshape(rows, t_cnt)

    def select_b(l, k):
        with jax.named_scope('select#l=%d,k=%d' % (l, k)):
            r = dot(smat[l], ag[:, :, cols(k)].reshape(ny * t_cnt, cw)).astype(BF)
            r = r.reshape(nd, ny * cap_e, cw)
            sel[l, :, :, cols(k)] = r
            xin[l, 0, :, cols(k)] = r[0]
            for dx, dc, _ in far_first:
                slot = ((nx - dx) % nx) * NC + dc
                send(sel.at[l, dx * NC + dc, :, cols(k)], xin.at[l, slot, :, cols(k)],
                     disp_send.at[l], disp_recv.at[l, k], (dx, dc, 0))

    def select_a(l):
        with jax.named_scope('select_a#l=%d' % l):
            r = dot(smata[l], xag[...].reshape(nx * t_cnt, aw)).astype(BF).reshape(NC * ny, nx * cap_e, aw)
            sela[l] = r
            xa[l, 0] = r[0]
            for _, dc, dj in col_far_first:
                slot = dc * ny + (ny - dj) % ny
                send(sela.at[l, dc * ny + dj], xa.at[l, slot], dispa_send.at[l], disp_recv.at[l, nk], (0, dc, dj))

    nw = ff // 2
    slots = {0: (0, 1), 1: (2, 0)}

    def up_proj(l, k, first=False, last=False):
        s1, s3 = slots[l]
        via_x = k < nk
        with jax.named_scope('wait_rows#l=%d,k=%d' % (l, k)):
            if via_x:
                wait_bytes(xin.at[l, pl.ds(1, nd - 1), :, cols(k)], disp_recv.at[l, k])
            else:
                wait_bytes(xa.at[l, pl.ds(1, NC * ny - 1)], disp_recv.at[l, k])
        if first:
            with jax.named_scope('wait_w13#l=%d' % l):
                wcopies['1_%d' % l].wait()
                wcopies['3_%d' % l].wait()
        with jax.named_scope('h#l=%d,k=%d' % (l, k)):
            if via_x:
                xp[...] = dot(perm[...], xin[l, :, :, cols(k)].reshape(rows, cw)).astype(BF)

            def body(n, carry):
                cs = pl.ds(pl.multiple_of(n * nw, nw), nw)
                if via_x:
                    xr, kr = xp[...], cols(k)
                else:
                    xr, kr = xa[l].reshape(rows, aw), pl.ds(bw, aw)
                d1 = dot(xr, wa[s1, kr, cs])
                d3 = dot(xr, wa[s3, kr, cs])
                if not first:
                    d1 = d1 + h1[:, cs]
                    d3 = d3 + h3[:, cs]
                if last:
                    act[:, cs] = (jax.nn.silu(d1) * d3).astype(BF)
                else:
                    h1[:, cs] = d1
                    h3[:, cs] = d3
                return carry

            lax.fori_loop(0, ff // nw, body, 0)

    def far(k):
        with jax.named_scope('wait_far#k=%d' % k):
            wait_bytes(ag.at[2, :, cols(k)], far_recv.at[k])

    lag = 5
    for k in range(nk):
        forward(k)
        if k + ahead < nk:
            send_own(k + ahead)
        if k == 1:
            with jax.named_scope('x_forward'):
                x_forward()
        if k >= 1:
            far(k - 1)
            select_b(0, k - 1)
        if k >= lag:
            up_proj(0, k - lag, first=k == lag)
    load_w('2_0', w2_hbm.at[0], wb, wb_sem.at[0])
    load_w('1_1', w1_hbm.at[1], wa.at[2], wa_sem.at[2])
    with jax.named_scope('wait_xfar'):
        wait_bytes(xag.at[2], xag_recv.at[2])
    select_a(0)
    far(nk - 1)
    select_b(0, nk - 1)
    select_a(1)
    select_b(1, 0)
    todo = list(range(nk - lag, nk - 1)) + [nk, nk - 1]
    for i, k in enumerate(todo):
        up_proj(0, k, last=i == len(todo) - 1)
        if i + 1 < nk:
            select_b(1, i + 1)
    for i in range(len(todo) + 1, nk):
        select_b(1, i)
    load_w('3_1', w3_hbm.at[1], wa.at[0], wa_sem.at[0])

    ck = [(o, min(nw2, d_model - o)) for o in range(0, d_model, nw2)]
    o_last, w_last = ck.pop()
    ck += [(o_last, w_last // 2), (o_last + w_last // 2, w_last // 2)]

    def down_proj(l):
        with jax.named_scope('wait_w2#l=%d' % l):
            wcopies['2_%d' % l].wait()
        for i, (o0, ow) in enumerate(ck):
            cs = pl.ds(o0, ow)
            with jax.named_scope('w2#l=%d,i=%d' % (l, i)):
                o = dot(act[...], wb[:, cs]).astype(BF).reshape(NC * ny, nx * cap_e, ow)
                out[l, :, :, cs] = o
                eb[0, l, :, cs] = o[0]
            for _, dc, dj in col_far_first:
                slot = dc * ny + (ny - dj) % ny
                send(out.at[l, dc * ny + dj, :, cs], eb.at[slot, l, :, cs],
                     comb_send.at[l], comb_recv.at[l, i], (0, dc, dj))

    down_proj(0)
    load_w('2_1', w2_hbm.at[1], wb, wb_sem.at[0])

    with jax.named_scope('wait_gates'):
        wait_bytes(xgates.at[pl.ds(1, nx - 1)], meta_recv.at[2])
    for rg in range(NC):
        e_vec = col_vecs[rg]
        gs_parts = []
        w_parts = [[], [], []]
        for s in range(nx):
            hit, key = col_key(rg, s)
            gate = jnp.zeros(e_vec.shape, F32)
            for m, u in picks:
                gate = jnp.where(xids[s, m, u:u + 1, :] == e_vec, xgates[s, m, u:u + 1, :], gate)
            any_hit = jnp.max(hit, axis=0, keepdims=True)
            g_hit = jnp.broadcast_to(any_hit, hit.shape)
            g_rank = dot(g_hit.astype(BF), upper)[0:1, :]
            g_key = jnp.where(any_hit > 0.0, g_rank + s * cap_g, -1.0)
            g_io = lax.broadcasted_iota(jnp.int32, (nx * cap_g, t_cnt), 0).astype(F32)
            gs_parts.append(jnp.where(g_key == g_io, 1.0, 0.0).astype(BF))
            g1 = gate.astype(BF)
            rest = gate - g1.astype(F32)
            g2 = rest.astype(BF)
            g3 = (rest - g2.astype(F32)).astype(BF)
            oh = one_hot(key, nx * cap_e)
            for part, gp in zip(w_parts, (g1, g2, g3)):
                w = jnp.where(oh, gp.astype(F32)[:, None, :], 0.0)
                part.append(w.astype(BF).reshape(e_grp * nx * cap_e, t_cnt))
        gs = jnp.concatenate(gs_parts, axis=1)
        n_g = nx * cap_g
        for i in range(3):
            w = jnp.concatenate(w_parts[i], axis=1)
            cmat[rg, i * n_g:(i + 1) * n_g, :] = dot_nt(gs, w).astype(BF)

    up_proj(1, nk, first=True)
    for k in range(nk):
        up_proj(1, k, last=k == nk - 1)
    down_proj(1)

    def merge(i):
        n_g = nx * cap_g
        cs, ow = pl.ds(*ck[i]), ck[i][1]
        for l in range(e_loc):
            with jax.named_scope('wait_comb#l=%d,i=%d' % (l, i)):
                wait_bytes(eb.at[pl.ds(1, NC * ny - 1), l, :, cs], comb_recv.at[l, i])
        with jax.named_scope('merge#i=%d' % i):
            for rg in range(NC):
                e = eb[rg * ny:(rg + 1) * ny, :, :, cs].reshape(ny * e_loc * nx * cap_e, ow)
                r = dot(cmat[rg], e)
                r = (r[0:n_g] + r[n_g:2 * n_g] + r[2 * n_g:3 * n_g]).astype(BF).reshape(nx, cap_g, ow)
                gsum[:, rg, :, cs] = r
                grec[0, rg, :, cs] = r[0]
            for dx in sorted(range(1, nx), key=lambda d: -min(d, nx - d)):
                send(gsum.at[dx, :, :, cs], grec.at[nx - dx, :, :, cs], fin_send, fin_recv.at[i], (dx, 0, 0))

    def final(i):
        cs, ow = pl.ds(*ck[i]), ck[i][1]
        with jax.named_scope('wait_fin#i=%d' % i):
            wait_bytes(grec.at[pl.ds(1, nx - 1), :, :, cs], fin_recv.at[i])
        with jax.named_scope('final#i=%d' % i):
            y_ref[:, cs] = dot(fmat[...], grec[:, :, :, cs].reshape(nd * cap_g, ow)).astype(BF)

    for i in range(len(ck)):
        merge(i)
    for i in range(len(ck)):
        final(i)

    wait_bytes(yids.at[pl.ds(1, ny - 1)], meta_send.at[0])
    wait_bytes(xids.at[pl.ds(1, nx - 1)], meta_send.at[1])
    wait_bytes(xgates.at[pl.ds(1, nx - 1)], meta_send.at[2])
    wait_bytes(ag.at[pl.ds(0, 2)], own_send)
    wait_bytes(ag.at[0], fwd_send)
    wait_bytes(xag.at[pl.ds(0, 2)], xag_send.at[0])
    wait_bytes(xag.at[0], xag_send.at[1])
    for l in range(e_loc):
        wait_bytes(sel.at[l, pl.ds(1, nd - 1)], disp_send.at[l])
        wait_bytes(sela.at[l, pl.ds(1, NC * ny - 1)], dispa_send.at[l])
        wait_bytes(out.at[l, pl.ds(1, NC * ny - 1)], comb_send.at[l])
    wait_bytes(gsum.at[pl.ds(1, nx - 1)], fin_send)


def solution(mesh):
    n_grp = mesh.shape['grp']
    ny = mesh.shape['ing']
    nx = n_grp // NC
    row_spec = P(('dp', 'grp', 'ing'))
    exp_spec = P(('grp', 'ing'))

    def local_fn(tokens, expert_ids, gate_vals, w_one, w_three, w_two):
        t_cnt, d_model = tokens.shape
        m_groups, per_group = expert_ids.shape[1:]
        e_loc, _, ff = w_one.shape
        e_grp = e_loc * ny
        cap_g = (t_cnt * m_groups + n_grp - 1) // n_grp
        cap_e = (cap_g * per_group + e_grp - 1) // e_grp
        cw, aw, nw2 = 256, 512, 512
        bw = d_model - aw
        nk = bw // cw
        ni = d_model // nw2 + 1
        rows = n_grp * ny * cap_e
        dims = (t_cnt, d_model, ff, nx, ny, e_loc, e_grp, cap_g, cap_e, cw, aw, nw2)

        ids_t = jnp.transpose(expert_ids, (1, 2, 0))
        gate_t = jnp.transpose(gate_vals, (1, 2, 0))

        vm, dma = pltpu.VMEM, pltpu.SemaphoreType.DMA
        hbm = pl.BlockSpec(memory_space=pltpu.HBM)
        vmem = pl.BlockSpec(memory_space=pltpu.VMEM)
        blk = nx * cap_e
        return pl.pallas_call(
            functools.partial(moe_kernel, dims),
            out_shape=jax.ShapeDtypeStruct((t_cnt, d_model), BF),
            in_specs=[hbm, vmem, vmem, hbm, hbm, hbm],
            out_specs=vmem,
            scratch_shapes=[
                vm((3, d_model, ff), BF), vm((ff, d_model), BF),
                vm((ny, t_cnt, bw), BF), vm((nx, t_cnt, aw), BF),
                vm((ny,) + ids_t.shape, jnp.int32), vm((nx,) + ids_t.shape, jnp.int32), vm((nx,) + ids_t.shape, F32),
                vm((e_loc, n_grp, ny * cap_e, bw), BF), vm((e_loc, NC * ny, blk, aw), BF),
                vm((e_loc, n_grp, ny * cap_e, bw), BF), vm((e_loc, NC * ny, blk, aw), BF),
                vm((rows, cw), BF), vm((rows, ff), F32), vm((rows, ff), F32), vm((rows, ff), BF),
                vm((e_loc, NC * ny, blk, d_model), BF), vm((NC * ny, e_loc, blk, d_model), BF),
                vm((nx, NC, cap_g, d_model), BF), vm((nx, NC, cap_g, d_model), BF),
                vm((rows, rows), BF), vm((e_loc, rows, ny * t_cnt), BF), vm((e_loc, rows, nx * t_cnt), BF),
                vm((NC, 3 * nx * cap_g, e_grp * blk), BF),
                vm((t_cnt, n_grp * cap_g), BF),
                dma((3,)), dma((1,)), dma((2,)), dma((3,)), dma((3,)),
                dma, dma, dma((nk,)), dma((nk,)), dma((nk,)),
                dma((2,)), dma((3,)), dma((e_loc,)), dma((e_loc,)), dma((e_loc, nk + 1)),
                dma((e_loc,)), dma((e_loc, ni)), dma, dma((ni,)),
            ],
            compiler_params=pltpu.CompilerParams(
                collective_id=0, has_side_effects=True, vmem_limit_bytes=67043328),
        )(tokens, ids_t, gate_t, w_one, w_three, w_two)

    return jax.shard_map(local_fn, mesh=mesh, in_specs=(row_spec, row_spec, row_spec, exp_spec, exp_spec, exp_spec), out_specs=row_spec, check_vma=False)
```

```python
import functools

import jax
import jax.numpy as jnp
from jax import lax
from jax.experimental import pallas as pl
from jax.experimental.pallas import tpu as pltpu
from jax.sharding import PartitionSpec as P

BF = jnp.bfloat16
F32 = jnp.float32
MESH = pl.DeviceIdType.MESH
NC = 2
NT = (((1,), (1,)), ((), ()))


def dot(a, b):
    return jnp.dot(a, b, preferred_element_type=F32)


def dot_nt(a, b):
    return lax.dot_general(a, b, NT, preferred_element_type=F32)


def wait_bytes(ref, sem):
    pltpu.make_async_copy(ref, ref, sem).wait()


def moe_kernel(dims, tok_hbm, ids_ref, gates_ref, w1_hbm, w3_hbm, w2_hbm, y_ref,
               wa, wb, ag, xag, yids, xids, xgates, sel, sela, xin, xa, xp, h1, h3, act, out, eb,
               gsum, grec, perm, smat, smata, cmat, fmat,
               wa_sem, wb_sem, tok_sem, meta_send, meta_recv,
               own_send, fwd_send, dn_recv, up_recv, far_recv,
               xag_send, xag_recv, disp_send, dispa_send, disp_recv, comb_send, comb_recv, fin_send, fin_recv):
    (t_cnt, d_model, ff, nx, ny, e_loc, e_grp, cap_g, cap_e, cw, aw, nw2) = dims
    m_groups, per_group, _ = ids_ref.shape
    picks = [(m, u) for m in range(m_groups) for u in range(per_group)]
    bw = d_model - aw
    nk = bw // cw
    nd = nx * NC
    rows = nd * ny * cap_e
    grp = lax.axis_index('grp')
    j = lax.axis_index('ing')
    x = grp // NC
    c = grp % NC

    def at(dx, dc, dj):
        gx = lax.rem(x + dx, nx)
        cc = c if dc == 0 else (NC - 1) - c
        return gx * NC + cc, lax.rem(j + dj, ny)

    def dev(dx, dc, dj):
        gg, jj = at(dx, dc, dj)
        return {'grp': gg, 'ing': jj}

    def send(src, dst, ssem, rsem, where):
        pltpu.make_async_remote_copy(src_ref=src, dst_ref=dst, send_sem=ssem, recv_sem=rsem,
                                     device_id=dev(*where), device_id_type=MESH).start()

    def cols(k):
        return pl.ds(k * cw, cw)

    row_peers = [(dx, dc, 0) for dx in range(nx) for dc in range(NC) if dx or dc]
    col_peers = [(0, dc, dj) for dj in range(ny) for dc in range(NC) if dj or dc]
    far_first = sorted(row_peers, key=lambda p: -min(p[0], nx - p[0]))
    col_far_first = sorted(col_peers, key=lambda p: -min(p[2], ny - p[2]))

    tok_cp = pltpu.make_async_copy(tok_hbm.at[:, pl.ds(0, bw)], ag.at[0], tok_sem.at[0])
    tok_cp.start()
    toka_cp = pltpu.make_async_copy(tok_hbm.at[:, pl.ds(bw, aw)], xag.at[0], tok_sem.at[1])
    toka_cp.start()
    wcopies = {}

    def load_w(name, src, dst, sem):
        cp = pltpu.make_async_copy(src, dst, sem)
        cp.start()
        wcopies[name] = cp

    barrier = pltpu.get_barrier_semaphore()
    peers = row_peers + [p for p in col_peers if p[2]]
    for p in peers:
        pl.semaphore_signal(barrier, inc=1, device_id=dev(*p), device_id_type=MESH)
    with jax.named_scope('barrier_wait'):
        pl.semaphore_wait(barrier, len(peers))
        tok_cp.wait()
        toka_cp.wait()

    for dj in range(1, ny):
        send(ids_ref, yids.at[ny - dj], meta_send.at[0], meta_recv.at[0], (0, 0, dj))
    for dx in range(1, nx):
        send(ids_ref, xids.at[nx - dx], meta_send.at[1], meta_recv.at[1], (dx, 0, 0))
        send(gates_ref, xgates.at[nx - dx], meta_send.at[2], meta_recv.at[2], (dx, 0, 0))

    def send_own(k):
        send(ag.at[0, :, cols(k)], ag.at[ny - 1, :, cols(k)], own_send, dn_recv.at[k], (0, 0, 1))
        send(ag.at[0, :, cols(k)], ag.at[1, :, cols(k)], own_send, up_recv.at[k], (0, 0, ny - 1))

    def forward(k):
        half = t_cnt // 2
        with jax.named_scope('wait_dn#k=%d' % k):
            wait_bytes(ag.at[ny - 1, :, cols(k)], dn_recv.at[k])
        src = ag.at[ny - 1, pl.ds(0, half), cols(k)]
        send(src, ag.at[2, pl.ds(0, half), cols(k)], fwd_send, far_recv.at[k], (0, 0, 1))
        with jax.named_scope('wait_up#k=%d' % k):
            wait_bytes(ag.at[1, :, cols(k)], up_recv.at[k])
        src = ag.at[1, pl.ds(half, half), cols(k)]
        send(src, ag.at[2, pl.ds(half, half), cols(k)], fwd_send, far_recv.at[k], (0, 0, ny - 1))

    ahead = 2
    for k in range(ahead):
        send_own(k)
    half = t_cnt // 2
    send(xag.at[0], xag.at[nx - 1], xag_send.at[0], xag_recv.at[0], (1, 0, 0))
    send(xag.at[0], xag.at[1], xag_send.at[0], xag_recv.at[1], (nx - 1, 0, 0))

    def x_forward():
        wait_bytes(xag.at[nx - 1], xag_recv.at[0])
        send(xag.at[nx - 1, pl.ds(0, half)], xag.at[2, pl.ds(0, half)], xag_send.at[1], xag_recv.at[2], (1, 0, 0))
        wait_bytes(xag.at[1], xag_recv.at[1])
        send(xag.at[1, pl.ds(half, half)], xag.at[2, pl.ds(half, half)], xag_send.at[1], xag_recv.at[2],
             (nx - 1, 0, 0))

    upper = (lax.broadcasted_iota(jnp.int32, (t_cnt, t_cnt), 0)
             < lax.broadcasted_iota(jnp.int32, (t_cnt, t_cnt), 1)).astype(F32).astype(BF)

    def vec_of(scalars):
        r_io = lax.broadcasted_iota(jnp.int32, (len(scalars), t_cnt), 0)
        v = jnp.zeros((len(scalars), t_cnt), jnp.int32)
        for r, s in enumerate(scalars):
            v = jnp.where(r_io == r, s, v)
        return v

    def chosen(ids, s, evec):
        hit = jnp.zeros(evec.shape, F32)
        for m, u in picks:
            hit = jnp.where(ids[s, m, u:u + 1, :] == evec, 1.0, hit)
        return hit

    def one_hot(key, n):
        m = key.shape[0]
        io = lax.broadcasted_iota(jnp.int32, (m, n, t_cnt), 1).astype(F32)
        return key[:, None, :] == io

    e_disp = []
    for l in range(e_loc):
        for dx in range(nx):
            for dc in range(NC):
                gg, jj = at(dx, dc, 0)
                e_disp.append(gg * e_grp + jj * e_loc + l)
    e_disp = vec_of(e_disp)

    g_lo = vec_of([at(dx, dc, 0)[0] * e_grp for dx in range(nx) for dc in range(NC)])
    hit = jnp.zeros(g_lo.shape, F32)
    for m, u in picks:
        row = ids_ref[m, u:u + 1, :]
        hit = jnp.where((row >= g_lo) & (row < g_lo + e_grp), 1.0, hit)
    key = jnp.where(hit > 0.0, dot(hit.astype(BF), upper), -1.0)
    ft = jnp.where(one_hot(key, cap_g), 1.0, 0.0).astype(BF).reshape(nd * cap_g, t_cnt)
    eye = (lax.broadcasted_iota(jnp.int32, (t_cnt, t_cnt), 0)
           == lax.broadcasted_iota(jnp.int32, (t_cnt, t_cnt), 1)).astype(F32).astype(BF)
    fmat[...] = dot_nt(eye, ft).astype(BF)

    yids[0] = ids_ref[...]
    xids[0] = ids_ref[...]
    xgates[0] = gates_ref[...]

    def split(v, n):
        hi = jnp.floor((v + 0.5) * (1.0 / n))
        return hi, v - hi * n

    blk_o, q_o = split(lax.broadcasted_iota(jnp.int32, (rows, rows), 0).astype(F32), cap_e)
    rest_o, rx_o = split(blk_o, nx)
    rc_o, rj_o = split(rest_o, ny)
    src = ((rx_o * NC + rc_o) * ny + rj_o) * cap_e + q_o
    src_io = lax.broadcasted_iota(jnp.int32, (rows, rows), 1).astype(F32)
    perm[...] = jnp.where(src == src_io, 1.0, 0.0).astype(BF)

    with jax.named_scope('wait_yids'):
        wait_bytes(yids.at[pl.ds(1, ny - 1)], meta_recv.at[0])
    load_w('1_0', w1_hbm.at[0], wa.at[0], wa_sem.at[0])
    load_w('3_0', w3_hbm.at[0], wa.at[1], wa_sem.at[1])
    for s in range(ny):
        hit = chosen(yids, s, e_disp)
        key = jnp.where(hit > 0.0, dot(hit.astype(BF), upper) + s * cap_e, -1.0)
        for l in range(e_loc):
            oh = jnp.where(one_hot(key[l * nd:(l + 1) * nd], ny * cap_e), 1.0, 0.0)
            smat[l, :, s * t_cnt:(s + 1) * t_cnt] = oh.astype(BF).reshape(rows, t_cnt)

    col_vecs = []
    for rg in range(NC):
        e_vec = []
        for dj in range(ny):
            for l in range(e_loc):
                gg, jj = at(0, rg, dj)
                e_vec.append(gg * e_grp + jj * e_loc + l)
        col_vecs.append(vec_of(e_vec))

    def col_key(rg, s):
        hit = chosen(xids, s, col_vecs[rg])
        return hit, jnp.where(hit > 0.0, dot(hit.astype(BF), upper) + s * cap_e, -1.0)

    with jax.named_scope('wait_xids'):
        wait_bytes(xids.at[pl.ds(1, nx - 1)], meta_recv.at[1])
    for s in range(nx):
        keys = [col_key(rg, s)[1] for rg in range(NC)]
        for l in range(e_loc):
            key = jnp.concatenate([keys[rg][dj * e_loc + l:dj * e_loc + l + 1]
                                   for rg in range(NC) for dj in range(ny)], axis=0)
            oh = jnp.where(one_hot(key, nx * cap_e), 1.0, 0.0)
            smata[l, :, s * t_cnt:(s + 1) * t_cnt] = oh.astype(BF).reshape(rows, t_cnt)

    def select_b(l, k):
        with jax.named_scope('select#l=%d,k=%d' % (l, k)):
            r = dot(smat[l], ag[:, :, cols(k)].reshape(ny * t_cnt, cw)).astype(BF)
            r = r.reshape(nd, ny * cap_e, cw)
            sel[l, :, :, cols(k)] = r
            xin[l, 0, :, cols(k)] = r[0]
            for dx, dc, _ in far_first:
                slot = ((nx - dx) % nx) * NC + dc
                send(sel.at[l, dx * NC + dc, :, cols(k)], xin.at[l, slot, :, cols(k)],
                     disp_send.at[l], disp_recv.at[l, k], (dx, dc, 0))

    def select_a(l):
        with jax.named_scope('select_a#l=%d' % l):
            r = dot(smata[l], xag[...].reshape(nx * t_cnt, aw)).astype(BF).reshape(NC * ny, nx * cap_e, aw)
            sela[l] = r
            xa[l, 0] = r[0]
            for _, dc, dj in col_far_first:
                slot = dc * ny + (ny - dj) % ny
                send(sela.at[l, dc * ny + dj], xa.at[l, slot], dispa_send.at[l], disp_recv.at[l, nk], (0, dc, dj))

    nw = ff // 2
    slots = {0: (0, 1), 1: (2, 0)}

    def up_proj(l, k, first=False, last=False):
        s1, s3 = slots[l]
        via_x = k < nk
        with jax.named_scope('wait_rows#l=%d,k=%d' % (l, k)):
            if via_x:
                wait_bytes(xin.at[l, pl.ds(1, nd - 1), :, cols(k)], disp_recv.at[l, k])
            else:
                wait_bytes(xa.at[l, pl.ds(1, NC * ny - 1)], disp_recv.at[l, k])
        if first:
            with jax.named_scope('wait_w13#l=%d' % l):
                wcopies['1_%d' % l].wait()
                wcopies['3_%d' % l].wait()
        with jax.named_scope('h#l=%d,k=%d' % (l, k)):
            if via_x:
                xp[...] = dot(perm[...], xin[l, :, :, cols(k)].reshape(rows, cw)).astype(BF)

            def body(n, carry):
                cs = pl.ds(pl.multiple_of(n * nw, nw), nw)
                if via_x:
                    xr, kr = xp[...], cols(k)
                else:
                    xr, kr = xa[l].reshape(rows, aw), pl.ds(bw, aw)
                d1 = dot(xr, wa[s1, kr, cs])
                d3 = dot(xr, wa[s3, kr, cs])
                if not first:
                    d1 = d1 + h1[:, cs]
                    d3 = d3 + h3[:, cs]
                if last:
                    act[:, cs] = (jax.nn.silu(d1) * d3).astype(BF)
                else:
                    h1[:, cs] = d1
                    h3[:, cs] = d3
                return carry

            lax.fori_loop(0, ff // nw, body, 0)

    def far(k):
        with jax.named_scope('wait_far#k=%d' % k):
            wait_bytes(ag.at[2, :, cols(k)], far_recv.at[k])

    for k in range(nk):
        forward(k)
        if k + ahead < nk:
            send_own(k + ahead)
        if k == 1:
            with jax.named_scope('x_forward'):
                x_forward()
        if k >= 1:
            far(k - 1)
            select_b(0, k - 1)
    load_w('2_0', w2_hbm.at[0], wb, wb_sem.at[0])
    load_w('1_1', w1_hbm.at[1], wa.at[2], wa_sem.at[2])
    with jax.named_scope('wait_xfar'):
        wait_bytes(xag.at[2], xag_recv.at[2])
    select_a(0)
    up_proj(0, 0, first=True)
    far(nk - 1)
    select_b(0, nk - 1)
    select_a(1)
    for k in range(1, nk - 1):
        up_proj(0, k)
        select_b(1, k - 1)
    up_proj(0, nk)
    up_proj(0, nk - 1, last=True)
    load_w('3_1', w3_hbm.at[1], wa.at[0], wa_sem.at[0])

    ck = [(o, min(nw2 // 2, d_model - o)) for o in range(0, d_model, nw2 // 2)]

    def down_proj(l, between=()):
        between = list(between)
        with jax.named_scope('wait_w2#l=%d' % l):
            wcopies['2_%d' % l].wait()
        for o0 in range(0, d_model, nw2):
            wide = pl.ds(o0, nw2)
            with jax.named_scope('w2#l=%d,o=%d' % (l, o0)):
                o = dot(act[...], wb[:, wide]).astype(BF).reshape(NC * ny, nx * cap_e, nw2)
                out[l, :, :, wide] = o
                eb[0, l, :, wide] = o[0]
            for i, (c0, ow) in enumerate(ck):
                if not o0 <= c0 < o0 + nw2:
                    continue
                cs = pl.ds(c0, ow)
                for _, dc, dj in col_far_first:
                    slot = dc * ny + (ny - dj) % ny
                    send(out.at[l, dc * ny + dj, :, cs], eb.at[slot, l, :, cs],
                         comb_send.at[l], comb_recv.at[l, i], (0, dc, dj))
            if between:
                between.pop(0)()

    down_proj(0, [functools.partial(select_b, 1, k) for k in range(nk - 2, nk)])
    load_w('2_1', w2_hbm.at[1], wb, wb_sem.at[0])

    with jax.named_scope('wait_gates'):
        wait_bytes(xgates.at[pl.ds(1, nx - 1)], meta_recv.at[2])
    for rg in range(NC):
        e_vec = col_vecs[rg]
        gs_parts = []
        w_parts = [[], [], []]
        for s in range(nx):
            hit, key = col_key(rg, s)
            gate = jnp.zeros(e_vec.shape, F32)
            for m, u in picks:
                gate = jnp.where(xids[s, m, u:u + 1, :] == e_vec, xgates[s, m, u:u + 1, :], gate)
            any_hit = jnp.max(hit, axis=0, keepdims=True)
            g_hit = jnp.broadcast_to(any_hit, hit.shape)
            g_rank = dot(g_hit.astype(BF), upper)[0:1, :]
            g_key = jnp.where(any_hit > 0.0, g_rank + s * cap_g, -1.0)
            g_io = lax.broadcasted_iota(jnp.int32, (nx * cap_g, t_cnt), 0).astype(F32)
            gs_parts.append(jnp.where(g_key == g_io, 1.0, 0.0).astype(BF))
            g1 = gate.astype(BF)
            rest = gate - g1.astype(F32)
            g2 = rest.astype(BF)
            g3 = (rest - g2.astype(F32)).astype(BF)
            oh = one_hot(key, nx * cap_e)
            for part, gp in zip(w_parts, (g1, g2, g3)):
                w = jnp.where(oh, gp.astype(F32)[:, None, :], 0.0)
                part.append(w.astype(BF).reshape(e_grp * nx * cap_e, t_cnt))
        gs = jnp.concatenate(gs_parts, axis=1)
        n_g = nx * cap_g
        for i in range(3):
            w = jnp.concatenate(w_parts[i], axis=1)
            cmat[rg, i * n_g:(i + 1) * n_g, :] = dot_nt(gs, w).astype(BF)

    up_proj(1, nk, first=True)
    for k in range(nk):
        up_proj(1, k, last=k == nk - 1)
    down_proj(1)

    def merge(i):
        n_g = nx * cap_g
        cs, ow = pl.ds(*ck[i]), ck[i][1]
        for l in range(e_loc):
            with jax.named_scope('wait_comb#l=%d,i=%d' % (l, i)):
                wait_bytes(eb.at[pl.ds(1, NC * ny - 1), l, :, cs], comb_recv.at[l, i])
        with jax.named_scope('merge#i=%d' % i):
            for rg in range(NC):
                e = eb[rg * ny:(rg + 1) * ny, :, :, cs].reshape(ny * e_loc * nx * cap_e, ow)
                r = dot(cmat[rg], e)
                r = (r[0:n_g] + r[n_g:2 * n_g] + r[2 * n_g:3 * n_g]).astype(BF).reshape(nx, cap_g, ow)
                gsum[:, rg, :, cs] = r
                grec[0, rg, :, cs] = r[0]
            for dx in sorted(range(1, nx), key=lambda d: -min(d, nx - d)):
                send(gsum.at[dx, :, :, cs], grec.at[nx - dx, :, :, cs], fin_send, fin_recv.at[i], (dx, 0, 0))

    def final(i):
        cs, ow = pl.ds(*ck[i]), ck[i][1]
        with jax.named_scope('wait_fin#i=%d' % i):
            wait_bytes(grec.at[pl.ds(1, nx - 1), :, :, cs], fin_recv.at[i])
        with jax.named_scope('final#i=%d' % i):
            y_ref[:, cs] = dot(fmat[...], grec[:, :, :, cs].reshape(nd * cap_g, ow)).astype(BF)

    for i in range(len(ck)):
        merge(i)
    for i in range(len(ck)):
        final(i)

    wait_bytes(yids.at[pl.ds(1, ny - 1)], meta_send.at[0])
    wait_bytes(xids.at[pl.ds(1, nx - 1)], meta_send.at[1])
    wait_bytes(xgates.at[pl.ds(1, nx - 1)], meta_send.at[2])
    wait_bytes(ag.at[pl.ds(0, 2)], own_send)
    wait_bytes(ag.at[0], fwd_send)
    wait_bytes(xag.at[pl.ds(0, 2)], xag_send.at[0])
    wait_bytes(xag.at[0], xag_send.at[1])
    for l in range(e_loc):
        wait_bytes(sel.at[l, pl.ds(1, nd - 1)], disp_send.at[l])
        wait_bytes(sela.at[l, pl.ds(1, NC * ny - 1)], dispa_send.at[l])
        wait_bytes(out.at[l, pl.ds(1, NC * ny - 1)], comb_send.at[l])
    wait_bytes(gsum.at[pl.ds(1, nx - 1)], fin_send)


def solution(mesh):
    n_grp = mesh.shape['grp']
    ny = mesh.shape['ing']
    nx = n_grp // NC
    row_spec = P(('dp', 'grp', 'ing'))
    exp_spec = P(('grp', 'ing'))

    def local_fn(tokens, expert_ids, gate_vals, w_one, w_three, w_two):
        t_cnt, d_model = tokens.shape
        m_groups, per_group = expert_ids.shape[1:]
        e_loc, _, ff = w_one.shape
        e_grp = e_loc * ny
        cap_g = (t_cnt * m_groups + n_grp - 1) // n_grp
        cap_e = (cap_g * per_group + e_grp - 1) // e_grp
        cw, aw, nw2 = 512, 512, 512
        bw = d_model - aw
        nk = bw // cw
        ni = d_model // (nw2 // 2)
        rows = n_grp * ny * cap_e
        dims = (t_cnt, d_model, ff, nx, ny, e_loc, e_grp, cap_g, cap_e, cw, aw, nw2)

        ids_t = jnp.transpose(expert_ids, (1, 2, 0))
        gate_t = jnp.transpose(gate_vals, (1, 2, 0))

        vm, dma = pltpu.VMEM, pltpu.SemaphoreType.DMA
        hbm = pl.BlockSpec(memory_space=pltpu.HBM)
        vmem = pl.BlockSpec(memory_space=pltpu.VMEM)
        blk = nx * cap_e
        return pl.pallas_call(
            functools.partial(moe_kernel, dims),
            out_shape=jax.ShapeDtypeStruct((t_cnt, d_model), BF),
            in_specs=[hbm, vmem, vmem, hbm, hbm, hbm],
            out_specs=vmem,
            scratch_shapes=[
                vm((3, d_model, ff), BF), vm((ff, d_model), BF),
                vm((ny, t_cnt, bw), BF), vm((nx, t_cnt, aw), BF),
                vm((ny,) + ids_t.shape, jnp.int32), vm((nx,) + ids_t.shape, jnp.int32), vm((nx,) + ids_t.shape, F32),
                vm((e_loc, n_grp, ny * cap_e, bw), BF), vm((e_loc, NC * ny, blk, aw), BF),
                vm((e_loc, n_grp, ny * cap_e, bw), BF), vm((e_loc, NC * ny, blk, aw), BF),
                vm((rows, cw), BF), vm((rows, ff), F32), vm((rows, ff), F32), vm((rows, ff), BF),
                vm((e_loc, NC * ny, blk, d_model), BF), vm((NC * ny, e_loc, blk, d_model), BF),
                vm((nx, NC, cap_g, d_model), BF), vm((nx, NC, cap_g, d_model), BF),
                vm((rows, rows), BF), vm((e_loc, rows, ny * t_cnt), BF), vm((e_loc, rows, nx * t_cnt), BF),
                vm((NC, 3 * nx * cap_g, e_grp * blk), BF),
                vm((t_cnt, n_grp * cap_g), BF),
                dma((3,)), dma((1,)), dma((2,)), dma((3,)), dma((3,)),
                dma, dma, dma((nk,)), dma((nk,)), dma((nk,)),
                dma((2,)), dma((3,)), dma((e_loc,)), dma((e_loc,)), dma((e_loc, nk + 1)),
                dma((e_loc,)), dma((e_loc, ni)), dma, dma((ni,)),
            ],
            compiler_params=pltpu.CompilerParams(
                collective_id=0, has_side_effects=True, vmem_limit_bytes=67043328),
        )(tokens, ids_t, gate_t, w_one, w_three, w_two)

    return jax.shard_map(local_fn, mesh=mesh, in_specs=(row_spec, row_spec, row_spec, exp_spec, exp_spec, exp_spec), out_specs=row_spec, check_vma=False)
```

```python
import functools

import jax
import jax.numpy as jnp
from jax import lax
from jax.experimental import pallas as pl
from jax.experimental.pallas import tpu as pltpu
from jax.sharding import PartitionSpec as P

BF = jnp.bfloat16
F32 = jnp.float32
MESH = pl.DeviceIdType.MESH
NC = 2
NT = (((1,), (1,)), ((), ()))


def dot(a, b):
    return jnp.dot(a, b, preferred_element_type=F32)


def dot_nt(a, b):
    return lax.dot_general(a, b, NT, preferred_element_type=F32)


def wait_bytes(ref, sem):
    pltpu.make_async_copy(ref, ref, sem).wait()


def moe_kernel(dims, tok_hbm, ids_ref, gates_ref, w1_hbm, w3_hbm, w2_hbm, grec, fmat,
               wa, wb, ag, xag, yids, xids, xgates, sel, sela, xin, xa, xp, h1, h3, act, out, eb,
               gsum, perm, smat, smata, cmat,
               wa_sem, wb_sem, tok_sem, meta_send, meta_recv,
               own_send, fwd_send, dn_recv, up_recv, far_recv,
               xag_send, xag_recv, disp_send, dispa_send, disp_recv, comb_send, comb_recv, fin_send, fin_recv, fin_own):
    (t_cnt, d_model, ff, nx, ny, e_loc, e_grp, cap_g, cap_e, cw, aw, nw2) = dims
    m_groups, per_group, _ = ids_ref.shape
    picks = [(m, u) for m in range(m_groups) for u in range(per_group)]
    bw = d_model - aw
    bk = [(o, min(cw, bw - o)) for o in range(0, bw, cw)]
    nk = len(bk)
    nd = nx * NC
    rows = nd * ny * cap_e
    grp = lax.axis_index('grp')
    j = lax.axis_index('ing')
    x = grp // NC
    c = grp % NC

    def at(dx, dc, dj):
        gx = lax.rem(x + dx, nx)
        cc = c if dc == 0 else (NC - 1) - c
        return gx * NC + cc, lax.rem(j + dj, ny)

    def dev(dx, dc, dj):
        gg, jj = at(dx, dc, dj)
        return {'grp': gg, 'ing': jj}

    def send(src, dst, ssem, rsem, where):
        pltpu.make_async_remote_copy(src_ref=src, dst_ref=dst, send_sem=ssem, recv_sem=rsem,
                                     device_id=dev(*where), device_id_type=MESH).start()

    def cols(k):
        return pl.ds(*bk[k])

    row_peers = [(dx, dc, 0) for dx in range(nx) for dc in range(NC) if dx or dc]
    col_peers = [(0, dc, dj) for dj in range(ny) for dc in range(NC) if dj or dc]
    far_first = sorted(row_peers, key=lambda p: -min(p[0], nx - p[0]))
    col_far_first = sorted(col_peers, key=lambda p: -min(p[2], ny - p[2]))

    tok_cp = pltpu.make_async_copy(tok_hbm.at[:, pl.ds(0, bw)], ag.at[0], tok_sem.at[0])
    tok_cp.start()
    toka_cp = pltpu.make_async_copy(tok_hbm.at[:, pl.ds(bw, aw)], xag.at[0], tok_sem.at[1])
    toka_cp.start()
    wcopies = {}

    def load_w(name, src, dst, sem):
        cp = pltpu.make_async_copy(src, dst, sem)
        cp.start()
        wcopies[name] = cp

    barrier = pltpu.get_barrier_semaphore()
    peers = row_peers + [p for p in col_peers if p[2]]
    for p in peers:
        pl.semaphore_signal(barrier, inc=1, device_id=dev(*p), device_id_type=MESH)
    with jax.named_scope('barrier_wait'):
        pl.semaphore_wait(barrier, len(peers))
        tok_cp.wait()
        toka_cp.wait()

    for dj in range(1, ny):
        send(ids_ref, yids.at[ny - dj], meta_send.at[0], meta_recv.at[0], (0, 0, dj))
    for dx in range(1, nx):
        send(ids_ref, xids.at[nx - dx], meta_send.at[1], meta_recv.at[1], (dx, 0, 0))
        send(gates_ref, xgates.at[nx - dx], meta_send.at[2], meta_recv.at[2], (dx, 0, 0))

    def send_own(k):
        send(ag.at[0, :, cols(k)], ag.at[ny - 1, :, cols(k)], own_send, dn_recv.at[k], (0, 0, 1))
        send(ag.at[0, :, cols(k)], ag.at[1, :, cols(k)], own_send, up_recv.at[k], (0, 0, ny - 1))

    def forward(k):
        half = t_cnt // 2
        with jax.named_scope('wait_dn#k=%d' % k):
            wait_bytes(ag.at[ny - 1, :, cols(k)], dn_recv.at[k])
        src = ag.at[ny - 1, pl.ds(0, half), cols(k)]
        send(src, ag.at[2, pl.ds(0, half), cols(k)], fwd_send, far_recv.at[k], (0, 0, 1))
        with jax.named_scope('wait_up#k=%d' % k):
            wait_bytes(ag.at[1, :, cols(k)], up_recv.at[k])
        src = ag.at[1, pl.ds(half, half), cols(k)]
        send(src, ag.at[2, pl.ds(half, half), cols(k)], fwd_send, far_recv.at[k], (0, 0, ny - 1))

    ahead = 2
    for k in range(ahead):
        send_own(k)
    half = t_cnt // 2
    send(xag.at[0], xag.at[nx - 1], xag_send.at[0], xag_recv.at[0], (1, 0, 0))
    send(xag.at[0], xag.at[1], xag_send.at[0], xag_recv.at[1], (nx - 1, 0, 0))

    def x_forward():
        wait_bytes(xag.at[nx - 1], xag_recv.at[0])
        send(xag.at[nx - 1, pl.ds(0, half)], xag.at[2, pl.ds(0, half)], xag_send.at[1], xag_recv.at[2], (1, 0, 0))
        wait_bytes(xag.at[1], xag_recv.at[1])
        send(xag.at[1, pl.ds(half, half)], xag.at[2, pl.ds(half, half)], xag_send.at[1], xag_recv.at[2],
             (nx - 1, 0, 0))

    upper = (lax.broadcasted_iota(jnp.int32, (t_cnt, t_cnt), 0)
             < lax.broadcasted_iota(jnp.int32, (t_cnt, t_cnt), 1)).astype(F32).astype(BF)

    def vec_of(scalars):
        r_io = lax.broadcasted_iota(jnp.int32, (len(scalars), t_cnt), 0)
        v = jnp.zeros((len(scalars), t_cnt), jnp.int32)
        for r, s in enumerate(scalars):
            v = jnp.where(r_io == r, s, v)
        return v

    def chosen(ids, s, evec):
        hit = jnp.zeros(evec.shape, F32)
        for m, u in picks:
            hit = jnp.where(ids[s, m, u:u + 1, :] == evec, 1.0, hit)
        return hit

    def one_hot(key, n):
        m = key.shape[0]
        io = lax.broadcasted_iota(jnp.int32, (m, n, t_cnt), 1).astype(F32)
        return key[:, None, :] == io

    e_disp = []
    for l in range(e_loc):
        for dx in range(nx):
            for dc in range(NC):
                gg, jj = at(dx, dc, 0)
                e_disp.append(gg * e_grp + jj * e_loc + l)
    e_disp = vec_of(e_disp)

    g_lo = vec_of([at(dx, dc, 0)[0] * e_grp for dx in range(nx) for dc in range(NC)])
    hit = jnp.zeros(g_lo.shape, F32)
    for m, u in picks:
        row = ids_ref[m, u:u + 1, :]
        hit = jnp.where((row >= g_lo) & (row < g_lo + e_grp), 1.0, hit)
    key = jnp.where(hit > 0.0, dot(hit.astype(BF), upper), -1.0)
    ft = jnp.where(one_hot(key, cap_g), 1.0, 0.0).astype(BF).reshape(nd * cap_g, t_cnt)
    eye = (lax.broadcasted_iota(jnp.int32, (t_cnt, t_cnt), 0)
           == lax.broadcasted_iota(jnp.int32, (t_cnt, t_cnt), 1)).astype(F32).astype(BF)
    fmat[...] = dot_nt(eye, ft).astype(BF)

    yids[0] = ids_ref[...]
    xids[0] = ids_ref[...]
    xgates[0] = gates_ref[...]

    def split(v, n):
        hi = jnp.floor((v + 0.5) * (1.0 / n))
        return hi, v - hi * n

    blk_o, q_o = split(lax.broadcasted_iota(jnp.int32, (rows, rows), 0).astype(F32), cap_e)
    rest_o, rx_o = split(blk_o, nx)
    rc_o, rj_o = split(rest_o, ny)
    src = ((rx_o * NC + rc_o) * ny + rj_o) * cap_e + q_o
    src_io = lax.broadcasted_iota(jnp.int32, (rows, rows), 1).astype(F32)
    perm[...] = jnp.where(src == src_io, 1.0, 0.0).astype(BF)

    with jax.named_scope('wait_yids'):
        wait_bytes(yids.at[pl.ds(1, ny - 1)], meta_recv.at[0])
    load_w('1_0', w1_hbm.at[0], wa.at[0], wa_sem.at[0])
    load_w('3_0', w3_hbm.at[0], wa.at[1], wa_sem.at[1])
    for s in range(ny):
        hit = chosen(yids, s, e_disp)
        key = jnp.where(hit > 0.0, dot(hit.astype(BF), upper) + s * cap_e, -1.0)
        for l in range(e_loc):
            oh = jnp.where(one_hot(key[l * nd:(l + 1) * nd], ny * cap_e), 1.0, 0.0)
            smat[l, :, s * t_cnt:(s + 1) * t_cnt] = oh.astype(BF).reshape(rows, t_cnt)

    col_vecs = []
    for rg in range(NC):
        e_vec = []
        for dj in range(ny):
            for l in range(e_loc):
                gg, jj = at(0, rg, dj)
                e_vec.append(gg * e_grp + jj * e_loc + l)
        col_vecs.append(vec_of(e_vec))

    def col_key(rg, s):
        hit = chosen(xids, s, col_vecs[rg])
        return hit, jnp.where(hit > 0.0, dot(hit.astype(BF), upper) + s * cap_e, -1.0)

    with jax.named_scope('wait_xids'):
        wait_bytes(xids.at[pl.ds(1, nx - 1)], meta_recv.at[1])
    for s in range(nx):
        keys = [col_key(rg, s)[1] for rg in range(NC)]
        for l in range(e_loc):
            key = jnp.concatenate([keys[rg][dj * e_loc + l:dj * e_loc + l + 1]
                                   for rg in range(NC) for dj in range(ny)], axis=0)
            oh = jnp.where(one_hot(key, nx * cap_e), 1.0, 0.0)
            smata[l, :, s * t_cnt:(s + 1) * t_cnt] = oh.astype(BF).reshape(rows, t_cnt)

    def select_b(l, k):
        with jax.named_scope('select#l=%d,k=%d' % (l, k)):
            r = dot(smat[l], ag[:, :, cols(k)].reshape(ny * t_cnt, bk[k][1])).astype(BF)
            r = r.reshape(nd, ny * cap_e, bk[k][1])
            sel[l, :, :, cols(k)] = r
            xin[l, 0, :, cols(k)] = r[0]
            for dx, dc, _ in far_first:
                slot = ((nx - dx) % nx) * NC + dc
                send(sel.at[l, dx * NC + dc, :, cols(k)], xin.at[l, slot, :, cols(k)],
                     disp_send.at[l], disp_recv.at[l, k], (dx, dc, 0))

    def select_a(l):
        with jax.named_scope('select_a#l=%d' % l):
            r = dot(smata[l], xag[...].reshape(nx * t_cnt, aw)).astype(BF).reshape(NC * ny, nx * cap_e, aw)
            sela[l] = r
            xa[l, 0] = r[0]
            for _, dc, dj in col_far_first:
                slot = dc * ny + (ny - dj) % ny
                send(sela.at[l, dc * ny + dj], xa.at[l, slot], dispa_send.at[l], disp_recv.at[l, nk], (0, dc, dj))

    slots = {0: (0, 1), 1: (2, 0)}

    def up_proj(l, k, first=False, last=False):
        s1, s3 = slots[l]
        via_x = k < nk
        with jax.named_scope('wait_rows#l=%d,k=%d' % (l, k)):
            if via_x:
                wait_bytes(xin.at[l, pl.ds(1, nd - 1), :, cols(k)], disp_recv.at[l, k])
            else:
                wait_bytes(xa.at[l, pl.ds(1, NC * ny - 1)], disp_recv.at[l, k])
        if first:
            with jax.named_scope('wait_w13#l=%d' % l):
                wcopies['1_%d' % l].wait()
                wcopies['3_%d' % l].wait()
        with jax.named_scope('h#l=%d,k=%d' % (l, k)):
            if via_x:
                w = bk[k][1]
                xp[:, 0:w] = dot(perm[...], xin[l, :, :, cols(k)].reshape(rows, w)).astype(BF)
            nw = ff // 2

            def body(n, carry):
                cs = pl.ds(pl.multiple_of(n * nw, nw), nw)
                if via_x:
                    xr, kr = xp[:, 0:w], cols(k)
                else:
                    xr, kr = xa[l].reshape(rows, aw), pl.ds(bw, aw)
                d1 = dot(xr, wa[s1, kr, cs])
                d3 = dot(xr, wa[s3, kr, cs])
                if not first:
                    d1 = d1 + h1[:, cs]
                    d3 = d3 + h3[:, cs]
                if last:
                    act[:, cs] = (jax.nn.silu(d1) * d3).astype(BF)
                else:
                    h1[:, cs] = d1
                    h3[:, cs] = d3
                return carry

            lax.fori_loop(0, ff // nw, body, 0)

    def far(k):
        with jax.named_scope('wait_far#k=%d' % k):
            wait_bytes(ag.at[2, :, cols(k)], far_recv.at[k])

    for k in range(nk):
        forward(k)
        if k + ahead < nk:
            send_own(k + ahead)
        if k == 1:
            with jax.named_scope('x_forward'):
                x_forward()
        if k >= 1:
            far(k - 1)
            select_b(0, k - 1)
    load_w('2_0', w2_hbm.at[0], wb, wb_sem.at[0])
    load_w('1_1', w1_hbm.at[1], wa.at[2], wa_sem.at[2])
    with jax.named_scope('wait_xfar'):
        wait_bytes(xag.at[2], xag_recv.at[2])
    select_a(0)
    far(nk - 1)
    select_b(0, nk - 1)
    up_proj(0, 0, first=True)
    select_a(1)
    up_proj(0, 1)
    select_b(1, 0)
    for k in range(2, nk - 1):
        up_proj(0, k)
    up_proj(0, nk)
    up_proj(0, nk - 1, last=True)
    load_w('3_1', w3_hbm.at[1], wa.at[0], wa_sem.at[0])

    ck = [(o, min(nw2 // 2, d_model - o)) for o in range(0, d_model, nw2 // 2)]

    def down_proj(l, between=()):
        between = list(between)
        with jax.named_scope('wait_w2#l=%d' % l):
            wcopies['2_%d' % l].wait()
        for o0 in range(0, d_model, nw2):
            wide = pl.ds(o0, nw2)
            with jax.named_scope('w2#l=%d,o=%d' % (l, o0)):
                o = dot(act[...], wb[:, wide]).astype(BF).reshape(NC * ny, nx * cap_e, nw2)
                out[l, :, :, wide] = o
                eb[0, l, :, wide] = o[0]
            for i, (c0, ow) in enumerate(ck):
                if not o0 <= c0 < o0 + nw2:
                    continue
                cs = pl.ds(c0, ow)
                for _, dc, dj in col_far_first:
                    slot = dc * ny + (ny - dj) % ny
                    send(out.at[l, dc * ny + dj, :, cs], eb.at[slot, l, :, cs],
                         comb_send.at[l], comb_recv.at[l, i], (0, dc, dj))
            if between:
                between.pop(0)()

    down_proj(0, [functools.partial(select_b, 1, k) for k in range(1, nk)])
    load_w('2_1', w2_hbm.at[1], wb, wb_sem.at[0])

    with jax.named_scope('wait_gates'):
        wait_bytes(xgates.at[pl.ds(1, nx - 1)], meta_recv.at[2])
    for rg in range(NC):
        e_vec = col_vecs[rg]
        gs_parts = []
        w_parts = [[], [], []]
        for s in range(nx):
            hit, key = col_key(rg, s)
            gate = jnp.zeros(e_vec.shape, F32)
            for m, u in picks:
                gate = jnp.where(xids[s, m, u:u + 1, :] == e_vec, xgates[s, m, u:u + 1, :], gate)
            any_hit = jnp.max(hit, axis=0, keepdims=True)
            g_hit = jnp.broadcast_to(any_hit, hit.shape)
            g_rank = dot(g_hit.astype(BF), upper)[0:1, :]
            g_key = jnp.where(any_hit > 0.0, g_rank + s * cap_g, -1.0)
            g_io = lax.broadcasted_iota(jnp.int32, (nx * cap_g, t_cnt), 0).astype(F32)
            gs_parts.append(jnp.where(g_key == g_io, 1.0, 0.0).astype(BF))
            g1 = gate.astype(BF)
            rest = gate - g1.astype(F32)
            g2 = rest.astype(BF)
            g3 = (rest - g2.astype(F32)).astype(BF)
            oh = one_hot(key, nx * cap_e)
            for part, gp in zip(w_parts, (g1, g2, g3)):
                w = jnp.where(oh, gp.astype(F32)[:, None, :], 0.0)
                part.append(w.astype(BF).reshape(e_grp * nx * cap_e, t_cnt))
        gs = jnp.concatenate(gs_parts, axis=1)
        n_g = nx * cap_g
        for i in range(3):
            w = jnp.concatenate(w_parts[i], axis=1)
            cmat[rg, i * n_g:(i + 1) * n_g, :] = dot_nt(gs, w).astype(BF)

    up_proj(1, nk, first=True)
    for k in range(nk):
        up_proj(1, k, last=k == nk - 1)
    down_proj(1)

    def merge(i):
        n_g = nx * cap_g
        cs, ow = pl.ds(*ck[i]), ck[i][1]
        for l in range(e_loc):
            with jax.named_scope('wait_comb#l=%d,i=%d' % (l, i)):
                wait_bytes(eb.at[pl.ds(1, NC * ny - 1), l, :, cs], comb_recv.at[l, i])
        with jax.named_scope('merge#i=%d' % i):
            for rg in range(NC):
                e = eb[rg * ny:(rg + 1) * ny, :, :, cs].reshape(ny * e_loc * nx * cap_e, ow)
                r = dot(cmat[rg], e)
                r = (r[0:n_g] + r[n_g:2 * n_g] + r[2 * n_g:3 * n_g]).astype(BF).reshape(nx, cap_g, ow)
                gsum[:, rg, :, cs] = r
            for dx in sorted(range(1, nx), key=lambda d: -min(d, nx - d)):
                send(gsum.at[dx, :, :, cs], grec.at[nx - dx, :, :, cs], fin_send, fin_recv, (dx, 0, 0))
            pltpu.make_async_copy(gsum.at[0, :, :, cs], grec.at[0, :, :, cs], fin_own).start()

    for i in range(len(ck)):
        merge(i)
    with jax.named_scope('wait_fin'):
        wait_bytes(grec.at[pl.ds(1, nx - 1)], fin_recv)
        wait_bytes(grec.at[0], fin_own)

    wait_bytes(yids.at[pl.ds(1, ny - 1)], meta_send.at[0])
    wait_bytes(xids.at[pl.ds(1, nx - 1)], meta_send.at[1])
    wait_bytes(xgates.at[pl.ds(1, nx - 1)], meta_send.at[2])
    wait_bytes(ag.at[pl.ds(0, 2)], own_send)
    wait_bytes(ag.at[0], fwd_send)
    wait_bytes(xag.at[pl.ds(0, 2)], xag_send.at[0])
    wait_bytes(xag.at[0], xag_send.at[1])
    for l in range(e_loc):
        wait_bytes(sel.at[l, pl.ds(1, nd - 1)], disp_send.at[l])
        wait_bytes(sela.at[l, pl.ds(1, NC * ny - 1)], dispa_send.at[l])
        wait_bytes(out.at[l, pl.ds(1, NC * ny - 1)], comb_send.at[l])
    wait_bytes(gsum.at[pl.ds(1, nx - 1)], fin_send)


def solution(mesh):
    n_grp = mesh.shape['grp']
    ny = mesh.shape['ing']
    nx = n_grp // NC
    row_spec = P(('dp', 'grp', 'ing'))
    exp_spec = P(('grp', 'ing'))

    def local_fn(tokens, expert_ids, gate_vals, w_one, w_three, w_two):
        t_cnt, d_model = tokens.shape
        m_groups, per_group = expert_ids.shape[1:]
        e_loc, _, ff = w_one.shape
        e_grp = e_loc * ny
        cap_g = (t_cnt * m_groups + n_grp - 1) // n_grp
        cap_e = (cap_g * per_group + e_grp - 1) // e_grp
        cw, aw, nw2 = 512, 768, 512
        bw = d_model - aw
        nk = (bw + cw - 1) // cw
        ni = d_model // (nw2 // 2)
        rows = n_grp * ny * cap_e
        dims = (t_cnt, d_model, ff, nx, ny, e_loc, e_grp, cap_g, cap_e, cw, aw, nw2)

        ids_t = jnp.transpose(expert_ids, (1, 2, 0))
        gate_t = jnp.transpose(gate_vals, (1, 2, 0))

        vm, dma = pltpu.VMEM, pltpu.SemaphoreType.DMA
        hbm = pl.BlockSpec(memory_space=pltpu.HBM)
        vmem = pl.BlockSpec(memory_space=pltpu.VMEM)
        blk = nx * cap_e
        sums, pick = pl.pallas_call(
            functools.partial(moe_kernel, dims),
            out_shape=[jax.ShapeDtypeStruct((nx, NC, cap_g, d_model), BF),
                       jax.ShapeDtypeStruct((t_cnt, n_grp * cap_g), BF)],
            in_specs=[hbm, vmem, vmem, hbm, hbm, hbm],
            out_specs=[hbm, vmem],
            scratch_shapes=[
                vm((3, d_model, ff), BF), vm((ff, d_model), BF),
                vm((ny, t_cnt, bw), BF), vm((nx, t_cnt, aw), BF),
                vm((ny,) + ids_t.shape, jnp.int32), vm((nx,) + ids_t.shape, jnp.int32), vm((nx,) + ids_t.shape, F32),
                vm((e_loc, n_grp, ny * cap_e, bw), BF), vm((e_loc, NC * ny, blk, aw), BF),
                vm((e_loc, n_grp, ny * cap_e, bw), BF), vm((e_loc, NC * ny, blk, aw), BF),
                vm((rows, cw), BF), vm((rows, ff), F32), vm((rows, ff), F32), vm((rows, ff), BF),
                vm((e_loc, NC * ny, blk, d_model), BF), vm((NC * ny, e_loc, blk, d_model), BF),
                vm((nx, NC, cap_g, d_model), BF),
                vm((rows, rows), BF), vm((e_loc, rows, ny * t_cnt), BF), vm((e_loc, rows, nx * t_cnt), BF),
                vm((NC, 3 * nx * cap_g, e_grp * blk), BF),
                dma((3,)), dma((1,)), dma((2,)), dma((3,)), dma((3,)),
                dma, dma, dma((nk,)), dma((nk,)), dma((nk,)),
                dma((2,)), dma((3,)), dma((e_loc,)), dma((e_loc,)), dma((e_loc, nk + 1)),
                dma((e_loc,)), dma((e_loc, ni)), dma, dma, dma,
            ],
            compiler_params=pltpu.CompilerParams(
                collective_id=0, has_side_effects=True, vmem_limit_bytes=67043328),
        )(tokens, ids_t, gate_t, w_one, w_three, w_two)
        sums = sums.reshape(n_grp * cap_g, d_model)
        return jnp.dot(pick, sums, preferred_element_type=F32).astype(BF)

    return jax.shard_map(local_fn, mesh=mesh, in_specs=(row_spec, row_spec, row_spec, exp_spec, exp_spec, exp_spec), out_specs=row_spec, check_vma=False)
```

```python
import functools

import jax
import jax.numpy as jnp
from jax import lax
from jax.experimental import pallas as pl
from jax.experimental.pallas import tpu as pltpu
from jax.sharding import PartitionSpec as P

BF = jnp.bfloat16
F32 = jnp.float32
MESH = pl.DeviceIdType.MESH
NC = 2
NT = (((1,), (1,)), ((), ()))


def dot(a, b):
    return jnp.dot(a, b, preferred_element_type=F32)


def dot_nt(a, b):
    return lax.dot_general(a, b, NT, preferred_element_type=F32)


def wait_bytes(ref, sem):
    pltpu.make_async_copy(ref, ref, sem).wait()


def moe_kernel(dims, tok_hbm, ids_ref, gates_ref, w1_hbm, w3_hbm, w2_hbm, grec, fmat,
               wa, wb, ag, xag, yids, xids, xgates, sel, sela, xin, xa, xp, h1, h3, act, out, eb,
               gsum, perm, smat, smata, cmat,
               wa_sem, wb_sem, tok_sem, meta_send, meta_recv,
               own_send, fwd_send, dn_recv, up_recv, far_recv,
               xag_send, xag_recv, disp_send, dispa_send, disp_recv, comb_send, comb_recv, fin_send, fin_recv):
    (t_cnt, d_model, ff, nx, ny, e_loc, e_grp, cap_g, cap_e, cw, aw, nw2) = dims
    m_groups, per_group, _ = ids_ref.shape
    picks = [(m, u) for m in range(m_groups) for u in range(per_group)]
    bw = d_model - aw
    bk = [(o, min(cw // 2, bw - o)) for o in range(0, bw, cw // 2)]
    wide = [(o, min(cw, bw - o)) for o in range(0, bw, cw)]
    nk, nw_k, via_y = len(bk), len(wide), -1
    nd = nx * NC
    rows = nd * ny * cap_e
    grp = lax.axis_index('grp')
    j = lax.axis_index('ing')
    x = grp // NC
    c = grp % NC

    def at(dx, dc, dj):
        gx = lax.rem(x + dx, nx)
        cc = c if dc == 0 else (NC - 1) - c
        return gx * NC + cc, lax.rem(j + dj, ny)

    def dev(dx, dc, dj):
        gg, jj = at(dx, dc, dj)
        return {'grp': gg, 'ing': jj}

    def send(src, dst, ssem, rsem, where):
        pltpu.make_async_remote_copy(src_ref=src, dst_ref=dst, send_sem=ssem, recv_sem=rsem,
                                     device_id=dev(*where), device_id_type=MESH).start()

    def cols(k):
        return pl.ds(*bk[k])

    row_peers = [(dx, dc, 0) for dx in range(nx) for dc in range(NC) if dx or dc]
    col_peers = [(0, dc, dj) for dj in range(ny) for dc in range(NC) if dj or dc]
    far_first = sorted(row_peers, key=lambda p: -min(p[0], nx - p[0]))
    col_far_first = sorted(col_peers, key=lambda p: -min(p[2], ny - p[2]))

    tok_cp = pltpu.make_async_copy(tok_hbm.at[:, pl.ds(0, bw)], ag.at[0], tok_sem.at[0])
    tok_cp.start()
    toka_cp = pltpu.make_async_copy(tok_hbm.at[:, pl.ds(bw, aw)], xag.at[0], tok_sem.at[1])
    toka_cp.start()
    wcopies = {}

    def load_w(name, src, dst, sem):
        cp = pltpu.make_async_copy(src, dst, sem)
        cp.start()
        wcopies[name] = cp

    barrier = pltpu.get_barrier_semaphore()
    peers = row_peers + [p for p in col_peers if p[2]]
    for p in peers:
        pl.semaphore_signal(barrier, inc=1, device_id=dev(*p), device_id_type=MESH)
    with jax.named_scope('barrier_wait'):
        pl.semaphore_wait(barrier, len(peers))
        tok_cp.wait()
        toka_cp.wait()

    for dj in range(1, ny):
        send(ids_ref, yids.at[ny - dj], meta_send.at[0], meta_recv.at[0], (0, 0, dj))
    for dx in range(1, nx):
        send(ids_ref, xids.at[nx - dx], meta_send.at[1], meta_recv.at[1], (dx, 0, 0))
        send(gates_ref, xgates.at[nx - dx], meta_send.at[2], meta_recv.at[2], (dx, 0, 0))

    def send_own(k):
        send(ag.at[0, :, cols(k)], ag.at[ny - 1, :, cols(k)], own_send, dn_recv.at[k], (0, 0, 1))
        send(ag.at[0, :, cols(k)], ag.at[1, :, cols(k)], own_send, up_recv.at[k], (0, 0, ny - 1))

    def forward(k):
        half = t_cnt // 2
        with jax.named_scope('wait_dn#k=%d' % k):
            wait_bytes(ag.at[ny - 1, :, cols(k)], dn_recv.at[k])
        src = ag.at[ny - 1, pl.ds(0, half), cols(k)]
        send(src, ag.at[2, pl.ds(0, half), cols(k)], fwd_send, far_recv.at[k], (0, 0, 1))
        with jax.named_scope('wait_up#k=%d' % k):
            wait_bytes(ag.at[1, :, cols(k)], up_recv.at[k])
        src = ag.at[1, pl.ds(half, half), cols(k)]
        send(src, ag.at[2, pl.ds(half, half), cols(k)], fwd_send, far_recv.at[k], (0, 0, ny - 1))

    ahead = 4
    for k in range(ahead):
        send_own(k)
    half = t_cnt // 2
    send(xag.at[0], xag.at[nx - 1], xag_send.at[0], xag_recv.at[0], (1, 0, 0))
    send(xag.at[0], xag.at[1], xag_send.at[0], xag_recv.at[1], (nx - 1, 0, 0))

    def x_forward():
        wait_bytes(xag.at[nx - 1], xag_recv.at[0])
        send(xag.at[nx - 1, pl.ds(0, half)], xag.at[2, pl.ds(0, half)], xag_send.at[1], xag_recv.at[2], (1, 0, 0))
        wait_bytes(xag.at[1], xag_recv.at[1])
        send(xag.at[1, pl.ds(half, half)], xag.at[2, pl.ds(half, half)], xag_send.at[1], xag_recv.at[2],
             (nx - 1, 0, 0))

    upper = (lax.broadcasted_iota(jnp.int32, (t_cnt, t_cnt), 0)
             < lax.broadcasted_iota(jnp.int32, (t_cnt, t_cnt), 1)).astype(F32).astype(BF)

    def vec_of(scalars):
        r_io = lax.broadcasted_iota(jnp.int32, (len(scalars), t_cnt), 0)
        v = jnp.zeros((len(scalars), t_cnt), jnp.int32)
        for r, s in enumerate(scalars):
            v = jnp.where(r_io == r, s, v)
        return v

    def chosen(ids, s, evec):
        hit = jnp.zeros(evec.shape, F32)
        for m, u in picks:
            hit = jnp.where(ids[s, m, u:u + 1, :] == evec, 1.0, hit)
        return hit

    def one_hot(key, n):
        m = key.shape[0]
        io = lax.broadcasted_iota(jnp.int32, (m, n, t_cnt), 1).astype(F32)
        return key[:, None, :] == io

    e_disp = []
    for l in range(e_loc):
        for dx in range(nx):
            for dc in range(NC):
                gg, jj = at(dx, dc, 0)
                e_disp.append(gg * e_grp + jj * e_loc + l)
    e_disp = vec_of(e_disp)

    g_lo = vec_of([at(dx, dc, 0)[0] * e_grp for dx in range(nx) for dc in range(NC)])
    hit = jnp.zeros(g_lo.shape, F32)
    for m, u in picks:
        row = ids_ref[m, u:u + 1, :]
        hit = jnp.where((row >= g_lo) & (row < g_lo + e_grp), 1.0, hit)
    key = jnp.where(hit > 0.0, dot(hit.astype(BF), upper), -1.0)
    ft = jnp.where(one_hot(key, cap_g), 1.0, 0.0).astype(BF).reshape(nd * cap_g, t_cnt)
    eye = (lax.broadcasted_iota(jnp.int32, (t_cnt, t_cnt), 0)
           == lax.broadcasted_iota(jnp.int32, (t_cnt, t_cnt), 1)).astype(F32).astype(BF)
    fmat[...] = dot_nt(eye, ft).astype(BF)

    yids[0] = ids_ref[...]
    xids[0] = ids_ref[...]
    xgates[0] = gates_ref[...]

    def split(v, n):
        hi = jnp.floor((v + 0.5) * (1.0 / n))
        return hi, v - hi * n

    blk_o, q_o = split(lax.broadcasted_iota(jnp.int32, (rows, rows), 0).astype(F32), cap_e)
    rest_o, rx_o = split(blk_o, nx)
    rc_o, rj_o = split(rest_o, ny)
    src = ((rx_o * NC + rc_o) * ny + rj_o) * cap_e + q_o
    src_io = lax.broadcasted_iota(jnp.int32, (rows, rows), 1).astype(F32)
    perm[...] = jnp.where(src == src_io, 1.0, 0.0).astype(BF)

    with jax.named_scope('wait_yids'):
        wait_bytes(yids.at[pl.ds(1, ny - 1)], meta_recv.at[0])
    load_w('1_0', w1_hbm.at[0], wa.at[0], wa_sem.at[0])
    load_w('3_0', w3_hbm.at[0], wa.at[1], wa_sem.at[1])
    for s in range(ny):
        hit = chosen(yids, s, e_disp)
        key = jnp.where(hit > 0.0, dot(hit.astype(BF), upper) + s * cap_e, -1.0)
        for l in range(e_loc):
            oh = jnp.where(one_hot(key[l * nd:(l + 1) * nd], ny * cap_e), 1.0, 0.0)
            smat[l, :, s * t_cnt:(s + 1) * t_cnt] = oh.astype(BF).reshape(rows, t_cnt)

    col_vecs = []
    for rg in range(NC):
        e_vec = []
        for dj in range(ny):
            for l in range(e_loc):
                gg, jj = at(0, rg, dj)
                e_vec.append(gg * e_grp + jj * e_loc + l)
        col_vecs.append(vec_of(e_vec))

    def col_key(rg, s):
        hit = chosen(xids, s, col_vecs[rg])
        return hit, jnp.where(hit > 0.0, dot(hit.astype(BF), upper) + s * cap_e, -1.0)

    with jax.named_scope('wait_xids'):
        wait_bytes(xids.at[pl.ds(1, nx - 1)], meta_recv.at[1])
    for s in range(nx):
        keys = [col_key(rg, s)[1] for rg in range(NC)]
        for l in range(e_loc):
            key = jnp.concatenate([keys[rg][dj * e_loc + l:dj * e_loc + l + 1]
                                   for rg in range(NC) for dj in range(ny)], axis=0)
            oh = jnp.where(one_hot(key, nx * cap_e), 1.0, 0.0)
            smata[l, :, s * t_cnt:(s + 1) * t_cnt] = oh.astype(BF).reshape(rows, t_cnt)

    def select_b(l, k):
        o, w = (bk if l == 0 else wide)[k]
        cs = pl.ds(o, w)
        with jax.named_scope('select#l=%d,k=%d' % (l, k)):
            r = dot(smat[l], ag[:, :, cs].reshape(ny * t_cnt, w)).astype(BF).reshape(nd, ny * cap_e, w)
            sel[l, :, :, cs] = r
            xin[l, 0, :, cs] = r[0]
            for dx, dc, _ in far_first:
                slot = ((nx - dx) % nx) * NC + dc
                send(sel.at[l, dx * NC + dc, :, cs], xin.at[l, slot, :, cs],
                     disp_send.at[l], disp_recv.at[l, k], (dx, dc, 0))

    def select_a(l):
        with jax.named_scope('select_a#l=%d' % l):
            r = dot(smata[l], xag[...].reshape(nx * t_cnt, aw)).astype(BF).reshape(NC * ny, nx * cap_e, aw)
            sela[l] = r
            xa[l, 0] = r[0]
            for _, dc, dj in col_far_first:
                slot = dc * ny + (ny - dj) % ny
                send(sela.at[l, dc * ny + dj], xa.at[l, slot], dispa_send.at[l], disp_recv.at[l, nk], (0, dc, dj))

    slots = {0: (0, 1), 1: (2, 0)}

    def up_proj(l, k, first=False, last=False):
        s1, s3 = slots[l]
        via_x = k != via_y
        o, w = wide[k] if via_x else (bw, aw)
        with jax.named_scope('wait_rows#l=%d,k=%d' % (l, k)):
            if not via_x:
                wait_bytes(xa.at[l, pl.ds(1, NC * ny - 1)], disp_recv.at[l, nk])
            else:
                for i, (po, pw) in enumerate(bk if l == 0 else wide):
                    if o <= po < o + w:
                        wait_bytes(xin.at[l, pl.ds(1, nd - 1), :, pl.ds(po, pw)], disp_recv.at[l, i])
        if first:
            with jax.named_scope('wait_w13#l=%d' % l):
                wcopies['1_%d' % l].wait()
                wcopies['3_%d' % l].wait()
        with jax.named_scope('h#l=%d,k=%d' % (l, k)):
            if via_x:
                xp[:, 0:w] = dot(perm[...], xin[l, :, :, pl.ds(o, w)].reshape(rows, w)).astype(BF)
            nw = ff // 2

            def body(n, carry):
                cs = pl.ds(pl.multiple_of(n * nw, nw), nw)
                if via_x:
                    xr, kr = xp[:, 0:w], pl.ds(o, w)
                else:
                    xr, kr = xa[l].reshape(rows, aw), pl.ds(bw, aw)
                d1 = dot(xr, wa[s1, kr, cs])
                d3 = dot(xr, wa[s3, kr, cs])
                if not first:
                    d1 = d1 + h1[:, cs]
                    d3 = d3 + h3[:, cs]
                if last:
                    act[:, cs] = (jax.nn.silu(d1) * d3).astype(BF)
                else:
                    h1[:, cs] = d1
                    h3[:, cs] = d3
                return carry

            lax.fori_loop(0, ff // nw, body, 0)

    def far(k):
        with jax.named_scope('wait_far#k=%d' % k):
            wait_bytes(ag.at[2, :, cols(k)], far_recv.at[k])

    for k in range(nk):
        forward(k)
        if k + ahead < nk:
            send_own(k + ahead)
        if k == 2:
            with jax.named_scope('x_forward'):
                x_forward()
        if k == nk - 2:
            up_proj(0, 0, first=True)
            load_w('2_0', w2_hbm.at[0], wb, wb_sem.at[0])
            load_w('1_1', w1_hbm.at[1], wa.at[2], wa_sem.at[2])
        if k == nk - 1:
            with jax.named_scope('wait_xfar'):
                wait_bytes(xag.at[2], xag_recv.at[2])
            select_a(0)
        if k >= 1:
            far(k - 1)
            select_b(0, k - 1)
    far(nk - 1)
    select_b(0, nk - 1)
    select_a(1)
    up_proj(0, 1)
    select_b(1, 0)
    for k in range(2, nw_k):
        up_proj(0, k)
    up_proj(0, via_y, last=True)
    load_w('3_1', w3_hbm.at[1], wa.at[0], wa_sem.at[0])

    ck = [(o, min(nw2 // 2, d_model - o)) for o in range(0, d_model, nw2 // 2)]

    def down_proj(l, between=()):
        between = list(between)
        with jax.named_scope('wait_w2#l=%d' % l):
            wcopies['2_%d' % l].wait()
        for o0 in range(0, d_model, nw2):
            w2s = pl.ds(o0, nw2)
            with jax.named_scope('w2#l=%d,o=%d' % (l, o0)):
                o = dot(act[...], wb[:, w2s]).astype(BF).reshape(NC * ny, nx * cap_e, nw2)
                out[l, :, :, w2s] = o
                eb[0, l, :, w2s] = o[0]
            for i, (c0, ow) in enumerate(ck):
                if not o0 <= c0 < o0 + nw2:
                    continue
                cs = pl.ds(c0, ow)
                for _, dc, dj in col_far_first:
                    slot = dc * ny + (ny - dj) % ny
                    send(out.at[l, dc * ny + dj, :, cs], eb.at[slot, l, :, cs],
                         comb_send.at[l], comb_recv.at[l, i], (0, dc, dj))
            if between:
                between.pop(0)()

    down_proj(0, [functools.partial(select_b, 1, k) for k in range(1, nw_k)])
    load_w('2_1', w2_hbm.at[1], wb, wb_sem.at[0])

    with jax.named_scope('wait_gates'):
        wait_bytes(xgates.at[pl.ds(1, nx - 1)], meta_recv.at[2])
    for rg in range(NC):
        e_vec = col_vecs[rg]
        gs_parts = []
        w_parts = [[], [], []]
        for s in range(nx):
            hit, key = col_key(rg, s)
            gate = jnp.zeros(e_vec.shape, F32)
            for m, u in picks:
                gate = jnp.where(xids[s, m, u:u + 1, :] == e_vec, xgates[s, m, u:u + 1, :], gate)
            any_hit = jnp.max(hit, axis=0, keepdims=True)
            g_hit = jnp.broadcast_to(any_hit, hit.shape)
            g_rank = dot(g_hit.astype(BF), upper)[0:1, :]
            g_key = jnp.where(any_hit > 0.0, g_rank + s * cap_g, -1.0)
            g_io = lax.broadcasted_iota(jnp.int32, (nx * cap_g, t_cnt), 0).astype(F32)
            gs_parts.append(jnp.where(g_key == g_io, 1.0, 0.0).astype(BF))
            g1 = gate.astype(BF)
            rest = gate - g1.astype(F32)
            g2 = rest.astype(BF)
            g3 = (rest - g2.astype(F32)).astype(BF)
            oh = one_hot(key, nx * cap_e)
            for part, gp in zip(w_parts, (g1, g2, g3)):
                w = jnp.where(oh, gp.astype(F32)[:, None, :], 0.0)
                part.append(w.astype(BF).reshape(e_grp * nx * cap_e, t_cnt))
        gs = jnp.concatenate(gs_parts, axis=1)
        n_g = nx * cap_g
        for i in range(3):
            w = jnp.concatenate(w_parts[i], axis=1)
            cmat[rg, i * n_g:(i + 1) * n_g, :] = dot_nt(gs, w).astype(BF)

    up_proj(1, via_y, first=True)
    for k in range(nw_k):
        up_proj(1, k, last=k == nw_k - 1)
    down_proj(1)

    def merge(i):
        n_g = nx * cap_g
        cs, ow = pl.ds(*ck[i]), ck[i][1]
        for l in range(e_loc):
            with jax.named_scope('wait_comb#l=%d,i=%d' % (l, i)):
                wait_bytes(eb.at[pl.ds(1, NC * ny - 1), l, :, cs], comb_recv.at[l, i])
        with jax.named_scope('merge#i=%d' % i):
            for rg in range(NC):
                e = eb[rg * ny:(rg + 1) * ny, :, :, cs].reshape(ny * e_loc * nx * cap_e, ow)
                r = dot(cmat[rg], e)
                r = (r[0:n_g] + r[n_g:2 * n_g] + r[2 * n_g:3 * n_g]).astype(BF).reshape(nx, cap_g, ow)
                gsum[:, rg, :, cs] = r
                grec[0, rg, :, cs] = r[0]
            for dx in sorted(range(1, nx), key=lambda d: -min(d, nx - d)):
                send(gsum.at[dx, :, :, cs], grec.at[nx - dx, :, :, cs], fin_send, fin_recv, (dx, 0, 0))

    for i in range(len(ck)):
        merge(i)
    with jax.named_scope('wait_fin'):
        wait_bytes(grec.at[pl.ds(1, nx - 1)], fin_recv)

    wait_bytes(yids.at[pl.ds(1, ny - 1)], meta_send.at[0])
    wait_bytes(xids.at[pl.ds(1, nx - 1)], meta_send.at[1])
    wait_bytes(xgates.at[pl.ds(1, nx - 1)], meta_send.at[2])
    wait_bytes(ag.at[pl.ds(0, 2)], own_send)
    wait_bytes(ag.at[0], fwd_send)
    wait_bytes(xag.at[pl.ds(0, 2)], xag_send.at[0])
    wait_bytes(xag.at[0], xag_send.at[1])
    for l in range(e_loc):
        wait_bytes(sel.at[l, pl.ds(1, nd - 1)], disp_send.at[l])
        wait_bytes(sela.at[l, pl.ds(1, NC * ny - 1)], dispa_send.at[l])
        wait_bytes(out.at[l, pl.ds(1, NC * ny - 1)], comb_send.at[l])
    wait_bytes(gsum.at[pl.ds(1, nx - 1)], fin_send)


def solution(mesh):
    n_grp = mesh.shape['grp']
    ny = mesh.shape['ing']
    nx = n_grp // NC
    row_spec = P(('dp', 'grp', 'ing'))
    exp_spec = P(('grp', 'ing'))

    def local_fn(tokens, expert_ids, gate_vals, w_one, w_three, w_two):
        t_cnt, d_model = tokens.shape
        m_groups, per_group = expert_ids.shape[1:]
        e_loc, _, ff = w_one.shape
        e_grp = e_loc * ny
        cap_g = (t_cnt * m_groups + n_grp - 1) // n_grp
        cap_e = (cap_g * per_group + e_grp - 1) // e_grp
        cw, aw, nw2 = 512, 768, 512
        bw = d_model - aw
        nk = (bw + cw // 2 - 1) // (cw // 2)
        ni = d_model // (nw2 // 2)
        rows = n_grp * ny * cap_e
        dims = (t_cnt, d_model, ff, nx, ny, e_loc, e_grp, cap_g, cap_e, cw, aw, nw2)

        ids_t = jnp.transpose(expert_ids, (1, 2, 0))
        gate_t = jnp.transpose(gate_vals, (1, 2, 0))

        vm, dma = pltpu.VMEM, pltpu.SemaphoreType.DMA
        hbm = pl.BlockSpec(memory_space=pltpu.HBM)
        vmem = pl.BlockSpec(memory_space=pltpu.VMEM)
        blk = nx * cap_e
        sums, pick = pl.pallas_call(
            functools.partial(moe_kernel, dims),
            out_shape=[vm((nx, NC, cap_g, d_model), BF), vm((t_cnt, n_grp * cap_g), BF)],
            in_specs=[hbm, vmem, vmem, hbm, hbm, hbm],
            out_specs=[vmem, vmem],
            scratch_shapes=[
                vm((3, d_model, ff), BF), vm((ff, d_model), BF),
                vm((ny, t_cnt, bw), BF), vm((nx, t_cnt, aw), BF),
                vm((ny,) + ids_t.shape, jnp.int32), vm((nx,) + ids_t.shape, jnp.int32), vm((nx,) + ids_t.shape, F32),
                vm((e_loc, n_grp, ny * cap_e, bw), BF), vm((e_loc, NC * ny, blk, aw), BF),
                vm((e_loc, n_grp, ny * cap_e, bw), BF), vm((e_loc, NC * ny, blk, aw), BF),
                vm((rows, cw), BF), vm((rows, ff), F32), vm((rows, ff), F32), vm((rows, ff), BF),
                vm((e_loc, NC * ny, blk, d_model), BF), vm((NC * ny, e_loc, blk, d_model), BF),
                vm((nx, NC, cap_g, d_model), BF),
                vm((rows, rows), BF), vm((e_loc, rows, ny * t_cnt), BF), vm((e_loc, rows, nx * t_cnt), BF),
                vm((NC, 3 * nx * cap_g, e_grp * blk), BF),
                dma((3,)), dma((1,)), dma((2,)), dma((3,)), dma((3,)),
                dma, dma, dma((nk,)), dma((nk,)), dma((nk,)),
                dma((2,)), dma((3,)), dma((e_loc,)), dma((e_loc,)), dma((e_loc, nk + 1)),
                dma((e_loc,)), dma((e_loc, ni)), dma, dma,
            ],
            compiler_params=pltpu.CompilerParams(
                collective_id=0, has_side_effects=True, vmem_limit_bytes=64800000),
        )(tokens, ids_t, gate_t, w_one, w_three, w_two)
        sums = sums.reshape(n_grp * cap_g, d_model)
        return jnp.dot(pick, sums, preferred_element_type=F32).astype(BF)

    return jax.shard_map(local_fn, mesh=mesh, in_specs=(row_spec, row_spec, row_spec, exp_spec, exp_spec, exp_spec), out_specs=row_spec, check_vma=False)
```

```python
import functools

import jax
import jax.numpy as jnp
from jax import lax
from jax.experimental import pallas as pl
from jax.experimental.pallas import tpu as pltpu
from jax.sharding import PartitionSpec as P

BF = jnp.bfloat16
F32 = jnp.float32
MESH = pl.DeviceIdType.MESH
NC = 2
NT = (((1,), (1,)), ((), ()))


def dot(a, b):
    return jnp.dot(a, b, preferred_element_type=F32)


def dot_nt(a, b):
    return lax.dot_general(a, b, NT, preferred_element_type=F32)


def wait_bytes(ref, sem):
    pltpu.make_async_copy(ref, ref, sem).wait()


def moe_kernel(dims, tok_hbm, ids_ref, gates_ref, w1_hbm, w3_hbm, w2_hbm, grec, fmat,
               wa, wb, ag, xag, yids, xids, xgates, sel, sela, xin, xa, xp, h1, h3, act, out, eb,
               gsum, perm, smat, smata, cmat,
               wa_sem, wb_sem, tok_sem, meta_send, meta_recv,
               own_send, fwd_send, dn_recv, up_recv, far_recv,
               xag_send, xag_recv, disp_send, dispa_send, disp_recv, comb_send, comb_recv, fin_send, fin_recv):
    (t_cnt, d_model, ff, nx, ny, e_loc, e_grp, cap_g, cap_e, cw, aw, nw2) = dims
    m_groups, per_group, _ = ids_ref.shape
    picks = [(m, u) for m in range(m_groups) for u in range(per_group)]
    bw = d_model - aw
    bk = [(o, min(cw, bw - o)) for o in range(0, bw, cw)]
    nk = len(bk)
    nd = nx * NC
    rows = nd * ny * cap_e
    grp = lax.axis_index('grp')
    j = lax.axis_index('ing')
    x = grp // NC
    c = grp % NC

    def at(dx, dc, dj):
        gx = lax.rem(x + dx, nx)
        cc = c if dc == 0 else (NC - 1) - c
        return gx * NC + cc, lax.rem(j + dj, ny)

    def dev(dx, dc, dj):
        gg, jj = at(dx, dc, dj)
        return {'grp': gg, 'ing': jj}

    def send(src, dst, ssem, rsem, where):
        pltpu.make_async_remote_copy(src_ref=src, dst_ref=dst, send_sem=ssem, recv_sem=rsem,
                                     device_id=dev(*where), device_id_type=MESH).start()

    def cols(k):
        return pl.ds(*bk[k])

    row_peers = [(dx, dc, 0) for dx in range(nx) for dc in range(NC) if dx or dc]
    col_peers = [(0, dc, dj) for dj in range(ny) for dc in range(NC) if dj or dc]
    far_first = sorted(row_peers, key=lambda p: -min(p[0], nx - p[0]))
    col_far_first = sorted(col_peers, key=lambda p: -min(p[2], ny - p[2]))

    tok_cp = pltpu.make_async_copy(tok_hbm.at[:, pl.ds(0, bw)], ag.at[0], tok_sem.at[0])
    tok_cp.start()
    toka_cp = pltpu.make_async_copy(tok_hbm.at[:, pl.ds(bw, aw)], xag.at[0], tok_sem.at[1])
    toka_cp.start()
    wcopies = {}

    def load_w(name, src, dst, sem):
        cp = pltpu.make_async_copy(src, dst, sem)
        cp.start()
        wcopies[name] = cp

    barrier = pltpu.get_barrier_semaphore()
    peers = row_peers + [p for p in col_peers if p[2]]
    for p in peers:
        pl.semaphore_signal(barrier, inc=1, device_id=dev(*p), device_id_type=MESH)
    with jax.named_scope('barrier_wait'):
        pl.semaphore_wait(barrier, len(peers))
        tok_cp.wait()
        toka_cp.wait()

    for dj in range(1, ny):
        send(ids_ref, yids.at[ny - dj], meta_send.at[0], meta_recv.at[0], (0, 0, dj))
    for dx in range(1, nx):
        send(ids_ref, xids.at[nx - dx], meta_send.at[1], meta_recv.at[1], (dx, 0, 0))
        send(gates_ref, xgates.at[nx - dx], meta_send.at[2], meta_recv.at[2], (dx, 0, 0))

    def send_own(k):
        send(ag.at[0, :, cols(k)], ag.at[ny - 1, :, cols(k)], own_send, dn_recv.at[k], (0, 0, 1))
        send(ag.at[0, :, cols(k)], ag.at[1, :, cols(k)], own_send, up_recv.at[k], (0, 0, ny - 1))

    def forward(k):
        half = t_cnt // 2
        with jax.named_scope('wait_dn#k=%d' % k):
            wait_bytes(ag.at[ny - 1, :, cols(k)], dn_recv.at[k])
        src = ag.at[ny - 1, pl.ds(0, half), cols(k)]
        send(src, ag.at[2, pl.ds(0, half), cols(k)], fwd_send, far_recv.at[k], (0, 0, 1))
        with jax.named_scope('wait_up#k=%d' % k):
            wait_bytes(ag.at[1, :, cols(k)], up_recv.at[k])
        src = ag.at[1, pl.ds(half, half), cols(k)]
        send(src, ag.at[2, pl.ds(half, half), cols(k)], fwd_send, far_recv.at[k], (0, 0, ny - 1))

    ahead = 2
    for k in range(ahead):
        send_own(k)
    half = t_cnt // 2
    send(xag.at[0], xag.at[nx - 1], xag_send.at[0], xag_recv.at[0], (1, 0, 0))
    send(xag.at[0], xag.at[1], xag_send.at[0], xag_recv.at[1], (nx - 1, 0, 0))

    def x_forward():
        wait_bytes(xag.at[nx - 1], xag_recv.at[0])
        send(xag.at[nx - 1, pl.ds(0, half)], xag.at[2, pl.ds(0, half)], xag_send.at[1], xag_recv.at[2], (1, 0, 0))
        wait_bytes(xag.at[1], xag_recv.at[1])
        send(xag.at[1, pl.ds(half, half)], xag.at[2, pl.ds(half, half)], xag_send.at[1], xag_recv.at[2],
             (nx - 1, 0, 0))

    upper = (lax.broadcasted_iota(jnp.int32, (t_cnt, t_cnt), 0)
             < lax.broadcasted_iota(jnp.int32, (t_cnt, t_cnt), 1)).astype(F32).astype(BF)

    def vec_of(scalars):
        r_io = lax.broadcasted_iota(jnp.int32, (len(scalars), t_cnt), 0)
        v = jnp.zeros((len(scalars), t_cnt), jnp.int32)
        for r, s in enumerate(scalars):
            v = jnp.where(r_io == r, s, v)
        return v

    def chosen(ids, s, evec):
        hit = jnp.zeros(evec.shape, F32)
        for m, u in picks:
            hit = jnp.where(ids[s, m, u:u + 1, :] == evec, 1.0, hit)
        return hit

    def one_hot(key, n):
        m = key.shape[0]
        io = lax.broadcasted_iota(jnp.int32, (m, n, t_cnt), 1).astype(F32)
        return key[:, None, :] == io

    e_disp = []
    for l in range(e_loc):
        for dx in range(nx):
            for dc in range(NC):
                gg, jj = at(dx, dc, 0)
                e_disp.append(gg * e_grp + jj * e_loc + l)
    e_disp = vec_of(e_disp)

    g_lo = vec_of([at(dx, dc, 0)[0] * e_grp for dx in range(nx) for dc in range(NC)])
    hit = jnp.zeros(g_lo.shape, F32)
    for m, u in picks:
        row = ids_ref[m, u:u + 1, :]
        hit = jnp.where((row >= g_lo) & (row < g_lo + e_grp), 1.0, hit)
    key = jnp.where(hit > 0.0, dot(hit.astype(BF), upper), -1.0)
    ft = jnp.where(one_hot(key, cap_g), 1.0, 0.0).astype(BF).reshape(nd * cap_g, t_cnt)
    eye = (lax.broadcasted_iota(jnp.int32, (t_cnt, t_cnt), 0)
           == lax.broadcasted_iota(jnp.int32, (t_cnt, t_cnt), 1)).astype(F32).astype(BF)
    fmat[...] = dot_nt(eye, ft).astype(BF)

    yids[0] = ids_ref[...]
    xids[0] = ids_ref[...]
    xgates[0] = gates_ref[...]

    def split(v, n):
        hi = jnp.floor((v + 0.5) * (1.0 / n))
        return hi, v - hi * n

    blk_o, q_o = split(lax.broadcasted_iota(jnp.int32, (rows, rows), 0).astype(F32), cap_e)
    rest_o, rx_o = split(blk_o, nx)
    rc_o, rj_o = split(rest_o, ny)
    src = ((rx_o * NC + rc_o) * ny + rj_o) * cap_e + q_o
    src_io = lax.broadcasted_iota(jnp.int32, (rows, rows), 1).astype(F32)
    perm[...] = jnp.where(src == src_io, 1.0, 0.0).astype(BF)

    with jax.named_scope('wait_yids'):
        wait_bytes(yids.at[pl.ds(1, ny - 1)], meta_recv.at[0])
    load_w('1_0', w1_hbm.at[0], wa.at[0], wa_sem.at[0])
    load_w('3_0', w3_hbm.at[0], wa.at[1], wa_sem.at[1])
    for s in range(ny):
        hit = chosen(yids, s, e_disp)
        key = jnp.where(hit > 0.0, dot(hit.astype(BF), upper) + s * cap_e, -1.0)
        for l in range(e_loc):
            oh = jnp.where(one_hot(key[l * nd:(l + 1) * nd], ny * cap_e), 1.0, 0.0)
            smat[l, :, s * t_cnt:(s + 1) * t_cnt] = oh.astype(BF).reshape(rows, t_cnt)

    col_vecs = []
    for rg in range(NC):
        e_vec = []
        for dj in range(ny):
            for l in range(e_loc):
                gg, jj = at(0, rg, dj)
                e_vec.append(gg * e_grp + jj * e_loc + l)
        col_vecs.append(vec_of(e_vec))

    def col_key(rg, s):
        hit = chosen(xids, s, col_vecs[rg])
        return hit, jnp.where(hit > 0.0, dot(hit.astype(BF), upper) + s * cap_e, -1.0)

    with jax.named_scope('wait_xids'):
        wait_bytes(xids.at[pl.ds(1, nx - 1)], meta_recv.at[1])
    for s in range(nx):
        keys = [col_key(rg, s)[1] for rg in range(NC)]
        for l in range(e_loc):
            key = jnp.concatenate([keys[rg][dj * e_loc + l:dj * e_loc + l + 1]
                                   for rg in range(NC) for dj in range(ny)], axis=0)
            oh = jnp.where(one_hot(key, nx * cap_e), 1.0, 0.0)
            smata[l, :, s * t_cnt:(s + 1) * t_cnt] = oh.astype(BF).reshape(rows, t_cnt)

    def select_b(l, k):
        with jax.named_scope('select#l=%d,k=%d' % (l, k)):
            r = dot(smat[l], ag[:, :, cols(k)].reshape(ny * t_cnt, bk[k][1])).astype(BF)
            r = r.reshape(nd, ny * cap_e, bk[k][1])
            sel[l, :, :, cols(k)] = r
            xin[l, 0, :, cols(k)] = r[0]
            for dx, dc, _ in far_first:
                slot = ((nx - dx) % nx) * NC + dc
                send(sel.at[l, dx * NC + dc, :, cols(k)], xin.at[l, slot, :, cols(k)],
                     disp_send.at[l], disp_recv.at[l, k], (dx, dc, 0))

    def select_a(l):
        with jax.named_scope('select_a#l=%d' % l):
            r = dot(smata[l], xag[...].reshape(nx * t_cnt, aw)).astype(BF).reshape(NC * ny, nx * cap_e, aw)
            sela[l] = r
            xa[l, 0] = r[0]
            for _, dc, dj in col_far_first:
                slot = dc * ny + (ny - dj) % ny
                send(sela.at[l, dc * ny + dj], xa.at[l, slot], dispa_send.at[l], disp_recv.at[l, nk], (0, dc, dj))

    slots = {0: (0, 1), 1: (2, 0)}

    def up_proj(l, k, first=False, last=False):
        s1, s3 = slots[l]
        via_x = k < nk
        with jax.named_scope('wait_rows#l=%d,k=%d' % (l, k)):
            if via_x:
                wait_bytes(xin.at[l, pl.ds(1, nd - 1), :, cols(k)], disp_recv.at[l, k])
            else:
                wait_bytes(xa.at[l, pl.ds(1, NC * ny - 1)], disp_recv.at[l, k])
        if first:
            with jax.named_scope('wait_w13#l=%d' % l):
                wcopies['1_%d' % l].wait()
                wcopies['3_%d' % l].wait()
        with jax.named_scope('h#l=%d,k=%d' % (l, k)):
            if via_x:
                w = bk[k][1]
                xp[:, 0:w] = dot(perm[...], xin[l, :, :, cols(k)].reshape(rows, w)).astype(BF)
            nw = ff // 2

            def body(n, carry):
                cs = pl.ds(pl.multiple_of(n * nw, nw), nw)
                if via_x:
                    xr, kr = xp[:, 0:w], cols(k)
                else:
                    xr, kr = xa[l].reshape(rows, aw), pl.ds(bw, aw)
                d1 = dot(xr, wa[s1, kr, cs])
                d3 = dot(xr, wa[s3, kr, cs])
                if not first:
                    d1 = d1 + h1[:, cs]
                    d3 = d3 + h3[:, cs]
                if last:
                    act[:, cs] = (jax.nn.silu(d1) * d3).astype(BF)
                else:
                    h1[:, cs] = d1
                    h3[:, cs] = d3
                return carry

            lax.fori_loop(0, ff // nw, body, 0)

    def far(k):
        with jax.named_scope('wait_far#k=%d' % k):
            wait_bytes(ag.at[2, :, cols(k)], far_recv.at[k])

    for k in range(nk):
        forward(k)
        if k + ahead < nk:
            send_own(k + ahead)
        if k == 1:
            with jax.named_scope('x_forward'):
                x_forward()
        if k >= 1:
            far(k - 1)
            select_b(0, k - 1)
    load_w('2_0', w2_hbm.at[0], wb, wb_sem.at[0])
    load_w('1_1', w1_hbm.at[1], wa.at[2], wa_sem.at[2])
    with jax.named_scope('wait_xfar'):
        wait_bytes(xag.at[2], xag_recv.at[2])
    select_a(0)
    far(nk - 1)
    select_b(0, nk - 1)
    up_proj(0, 0, first=True)
    select_a(1)
    up_proj(0, 1)
    select_b(1, 0)
    for k in range(2, nk - 1):
        up_proj(0, k)
    up_proj(0, nk)
    up_proj(0, nk - 1, last=True)
    load_w('3_1', w3_hbm.at[1], wa.at[0], wa_sem.at[0])

    ck = [(o, min(nw2 // 2, d_model - o)) for o in range(0, d_model, nw2 // 2)]
    o_last, w_last = ck.pop()
    ck += [(o_last, w_last // 2), (o_last + w_last // 2, w_last // 2)]

    def down_proj(l, between=()):
        between = list(between)
        with jax.named_scope('wait_w2#l=%d' % l):
            wcopies['2_%d' % l].wait()
        for o0 in range(0, d_model, nw2):
            wide = pl.ds(o0, nw2)
            with jax.named_scope('w2#l=%d,o=%d' % (l, o0)):
                o = dot(act[...], wb[:, wide]).astype(BF).reshape(NC * ny, nx * cap_e, nw2)
                out[l, :, :, wide] = o
                eb[0, l, :, wide] = o[0]
            for i, (c0, ow) in enumerate(ck):
                if not o0 <= c0 < o0 + nw2:
                    continue
                cs = pl.ds(c0, ow)
                for _, dc, dj in col_far_first:
                    slot = dc * ny + (ny - dj) % ny
                    send(out.at[l, dc * ny + dj, :, cs], eb.at[slot, l, :, cs],
                         comb_send.at[l], comb_recv.at[l, i], (0, dc, dj))
            if between:
                between.pop(0)()

    down_proj(0, [functools.partial(select_b, 1, k) for k in range(1, nk)])
    load_w('2_1', w2_hbm.at[1], wb, wb_sem.at[0])

    with jax.named_scope('wait_gates'):
        wait_bytes(xgates.at[pl.ds(1, nx - 1)], meta_recv.at[2])
    for rg in range(NC):
        e_vec = col_vecs[rg]
        gs_parts = []
        w_parts = [[], [], []]
        for s in range(nx):
            hit, key = col_key(rg, s)
            gate = jnp.zeros(e_vec.shape, F32)
            for m, u in picks:
                gate = jnp.where(xids[s, m, u:u + 1, :] == e_vec, xgates[s, m, u:u + 1, :], gate)
            any_hit = jnp.max(hit, axis=0, keepdims=True)
            g_hit = jnp.broadcast_to(any_hit, hit.shape)
            g_rank = dot(g_hit.astype(BF), upper)[0:1, :]
            g_key = jnp.where(any_hit > 0.0, g_rank + s * cap_g, -1.0)
            g_io = lax.broadcasted_iota(jnp.int32, (nx * cap_g, t_cnt), 0).astype(F32)
            gs_parts.append(jnp.where(g_key == g_io, 1.0, 0.0).astype(BF))
            g1 = gate.astype(BF)
            rest = gate - g1.astype(F32)
            g2 = rest.astype(BF)
            g3 = (rest - g2.astype(F32)).astype(BF)
            oh = one_hot(key, nx * cap_e)
            for part, gp in zip(w_parts, (g1, g2, g3)):
                w = jnp.where(oh, gp.astype(F32)[:, None, :], 0.0)
                part.append(w.astype(BF).reshape(e_grp * nx * cap_e, t_cnt))
        gs = jnp.concatenate(gs_parts, axis=1)
        n_g = nx * cap_g
        for i in range(3):
            w = jnp.concatenate(w_parts[i], axis=1)
            cmat[rg, i * n_g:(i + 1) * n_g, :] = dot_nt(gs, w).astype(BF)

    up_proj(1, nk, first=True)
    for k in range(nk):
        up_proj(1, k, last=k == nk - 1)
    down_proj(1)

    def merge(i):
        n_g = nx * cap_g
        cs, ow = pl.ds(*ck[i]), ck[i][1]
        for l in range(e_loc):
            with jax.named_scope('wait_comb#l=%d,i=%d' % (l, i)):
                wait_bytes(eb.at[pl.ds(1, NC * ny - 1), l, :, cs], comb_recv.at[l, i])
        with jax.named_scope('merge#i=%d' % i):
            for rg in range(NC):
                e = eb[rg * ny:(rg + 1) * ny, :, :, cs].reshape(ny * e_loc * nx * cap_e, ow)
                r = dot(cmat[rg], e)
                r = (r[0:n_g] + r[n_g:2 * n_g] + r[2 * n_g:3 * n_g]).astype(BF).reshape(nx, cap_g, ow)
                gsum[:, rg, :, cs] = r
                grec[0, rg, :, cs] = r[0]
            for dx in sorted(range(1, nx), key=lambda d: -min(d, nx - d)):
                send(gsum.at[dx, :, :, cs], grec.at[nx - dx, :, :, cs], fin_send, fin_recv, (dx, 0, 0))

    for i in range(len(ck)):
        merge(i)
    with jax.named_scope('wait_fin'):
        wait_bytes(grec.at[pl.ds(1, nx - 1)], fin_recv)

    wait_bytes(yids.at[pl.ds(1, ny - 1)], meta_send.at[0])
    wait_bytes(xids.at[pl.ds(1, nx - 1)], meta_send.at[1])
    wait_bytes(xgates.at[pl.ds(1, nx - 1)], meta_send.at[2])
    wait_bytes(ag.at[pl.ds(0, 2)], own_send)
    wait_bytes(ag.at[0], fwd_send)
    wait_bytes(xag.at[pl.ds(0, 2)], xag_send.at[0])
    wait_bytes(xag.at[0], xag_send.at[1])
    for l in range(e_loc):
        wait_bytes(sel.at[l, pl.ds(1, nd - 1)], disp_send.at[l])
        wait_bytes(sela.at[l, pl.ds(1, NC * ny - 1)], dispa_send.at[l])
        wait_bytes(out.at[l, pl.ds(1, NC * ny - 1)], comb_send.at[l])
    wait_bytes(gsum.at[pl.ds(1, nx - 1)], fin_send)


def solution(mesh):
    n_grp = mesh.shape['grp']
    ny = mesh.shape['ing']
    nx = n_grp // NC
    row_spec = P(('dp', 'grp', 'ing'))
    exp_spec = P(('grp', 'ing'))

    def local_fn(tokens, expert_ids, gate_vals, w_one, w_three, w_two):
        t_cnt, d_model = tokens.shape
        m_groups, per_group = expert_ids.shape[1:]
        e_loc, _, ff = w_one.shape
        e_grp = e_loc * ny
        cap_g = (t_cnt * m_groups + n_grp - 1) // n_grp
        cap_e = (cap_g * per_group + e_grp - 1) // e_grp
        cw, aw, nw2 = 512, 768, 512
        bw = d_model - aw
        nk = (bw + cw - 1) // cw
        ni = d_model // (nw2 // 2) + 1
        rows = n_grp * ny * cap_e
        dims = (t_cnt, d_model, ff, nx, ny, e_loc, e_grp, cap_g, cap_e, cw, aw, nw2)

        ids_t = jnp.transpose(expert_ids, (1, 2, 0))
        gate_t = jnp.transpose(gate_vals, (1, 2, 0))

        vm, dma = pltpu.VMEM, pltpu.SemaphoreType.DMA
        hbm = pl.BlockSpec(memory_space=pltpu.HBM)
        vmem = pl.BlockSpec(memory_space=pltpu.VMEM)
        blk = nx * cap_e
        sums, pick = pl.pallas_call(
            functools.partial(moe_kernel, dims),
            out_shape=[vm((nx, NC, cap_g, d_model), BF), vm((t_cnt, n_grp * cap_g), BF)],
            in_specs=[hbm, vmem, vmem, hbm, hbm, hbm],
            out_specs=[vmem, vmem],
            scratch_shapes=[
                vm((3, d_model, ff), BF), vm((ff, d_model), BF),
                vm((ny, t_cnt, bw), BF), vm((nx, t_cnt, aw), BF),
                vm((ny,) + ids_t.shape, jnp.int32), vm((nx,) + ids_t.shape, jnp.int32), vm((nx,) + ids_t.shape, F32),
                vm((e_loc, n_grp, ny * cap_e, bw), BF), vm((e_loc, NC * ny, blk, aw), BF),
                vm((e_loc, n_grp, ny * cap_e, bw), BF), vm((e_loc, NC * ny, blk, aw), BF),
                vm((rows, cw), BF), vm((rows, ff), F32), vm((rows, ff), F32), vm((rows, ff), BF),
                vm((e_loc, NC * ny, blk, d_model), BF), vm((NC * ny, e_loc, blk, d_model), BF),
                vm((nx, NC, cap_g, d_model), BF),
                vm((rows, rows), BF), vm((e_loc, rows, ny * t_cnt), BF), vm((e_loc, rows, nx * t_cnt), BF),
                vm((NC, 3 * nx * cap_g, e_grp * blk), BF),
                dma((3,)), dma((1,)), dma((2,)), dma((3,)), dma((3,)),
                dma, dma, dma((nk,)), dma((nk,)), dma((nk,)),
                dma((2,)), dma((3,)), dma((e_loc,)), dma((e_loc,)), dma((e_loc, nk + 1)),
                dma((e_loc,)), dma((e_loc, ni)), dma, dma,
            ],
            compiler_params=pltpu.CompilerParams(
                collective_id=0, has_side_effects=True, vmem_limit_bytes=64800000),
        )(tokens, ids_t, gate_t, w_one, w_three, w_two)
        sums = sums.reshape(n_grp * cap_g, d_model)
        return jnp.dot(pick, sums, preferred_element_type=F32).astype(BF)

    return jax.shard_map(local_fn, mesh=mesh, in_specs=(row_spec, row_spec, row_spec, exp_spec, exp_spec, exp_spec), out_specs=row_spec, check_vma=False)
```

```python
import functools

import jax
import jax.numpy as jnp
from jax import lax
from jax.experimental import pallas as pl
from jax.experimental.pallas import tpu as pltpu
from jax.sharding import PartitionSpec as P

BF = jnp.bfloat16
F32 = jnp.float32
MESH = pl.DeviceIdType.MESH
NC = 2
NT = (((1,), (1,)), ((), ()))


def dot(a, b):
    return jnp.dot(a, b, preferred_element_type=F32)


def dot_nt(a, b):
    return lax.dot_general(a, b, NT, preferred_element_type=F32)


def wait_bytes(ref, sem):
    pltpu.make_async_copy(ref, ref, sem).wait()


def moe_kernel(dims, tok_hbm, ids_ref, gates_ref, w1_hbm, w3_hbm, w2_hbm, grec, fmat,
               wa, wb, ag, xag, yids, xids, xgates, sel, sela, xin, xa, xp, h1, h3, act, out, eb,
               gsum, perm, smat, smata, cmat,
               wa_sem, wb_sem, tok_sem, meta_send, meta_recv,
               own_send, fwd_send, dn_recv, up_recv, far_recv,
               xag_send, xag_recv, disp_send, dispa_send, disp_recv, comb_send, comb_recv, fin_send, fin_recv):
    (t_cnt, d_model, ff, nx, ny, e_loc, e_grp, cap_g, cap_e, cw, aw, nw2) = dims
    m_groups, per_group, _ = ids_ref.shape
    picks = [(m, u) for m in range(m_groups) for u in range(per_group)]
    bw = d_model - aw
    bk = [(o, min(cw, bw - o)) for o in range(0, bw, cw)]
    nk = len(bk)
    nd = nx * NC
    rows = nd * ny * cap_e
    grp = lax.axis_index('grp')
    j = lax.axis_index('ing')
    x = grp // NC
    c = grp % NC

    def at(dx, dc, dj):
        gx = lax.rem(x + dx, nx)
        cc = c if dc == 0 else (NC - 1) - c
        return gx * NC + cc, lax.rem(j + dj, ny)

    def dev(dx, dc, dj):
        gg, jj = at(dx, dc, dj)
        return {'grp': gg, 'ing': jj}

    def send(src, dst, ssem, rsem, where):
        pltpu.make_async_remote_copy(src_ref=src, dst_ref=dst, send_sem=ssem, recv_sem=rsem,
                                     device_id=dev(*where), device_id_type=MESH).start()

    def cols(k):
        return pl.ds(*bk[k])

    row_peers = [(dx, dc, 0) for dx in range(nx) for dc in range(NC) if dx or dc]
    col_peers = [(0, dc, dj) for dj in range(ny) for dc in range(NC) if dj or dc]
    far_first = sorted(row_peers, key=lambda p: -min(p[0], nx - p[0]))
    col_far_first = sorted(col_peers, key=lambda p: -min(p[2], ny - p[2]))

    tok_cp = pltpu.make_async_copy(tok_hbm.at[:, pl.ds(0, bw)], ag.at[0], tok_sem.at[0])
    tok_cp.start()
    toka_cp = pltpu.make_async_copy(tok_hbm.at[:, pl.ds(bw, aw)], xag.at[0], tok_sem.at[1])
    toka_cp.start()
    wcopies = {}

    def load_w(name, src, dst, sem):
        cp = pltpu.make_async_copy(src, dst, sem)
        cp.start()
        wcopies[name] = cp

    barrier = pltpu.get_barrier_semaphore()
    peers = row_peers + [p for p in col_peers if p[2]]
    for p in peers:
        pl.semaphore_signal(barrier, inc=1, device_id=dev(*p), device_id_type=MESH)
    with jax.named_scope('barrier_wait'):
        pl.semaphore_wait(barrier, len(peers))
        tok_cp.wait()
        toka_cp.wait()

    for dj in range(1, ny):
        send(ids_ref, yids.at[ny - dj], meta_send.at[0], meta_recv.at[0], (0, 0, dj))
    for dx in range(1, nx):
        send(ids_ref, xids.at[nx - dx], meta_send.at[1], meta_recv.at[1], (dx, 0, 0))
        send(gates_ref, xgates.at[nx - dx], meta_send.at[2], meta_recv.at[2], (dx, 0, 0))

    def send_own(k):
        send(ag.at[0, :, cols(k)], ag.at[ny - 1, :, cols(k)], own_send, dn_recv.at[k], (0, 0, 1))
        send(ag.at[0, :, cols(k)], ag.at[1, :, cols(k)], own_send, up_recv.at[k], (0, 0, ny - 1))

    def forward(k):
        half = t_cnt // 2
        with jax.named_scope('wait_dn#k=%d' % k):
            wait_bytes(ag.at[ny - 1, :, cols(k)], dn_recv.at[k])
        src = ag.at[ny - 1, pl.ds(0, half), cols(k)]
        send(src, ag.at[2, pl.ds(0, half), cols(k)], fwd_send, far_recv.at[k], (0, 0, 1))
        with jax.named_scope('wait_up#k=%d' % k):
            wait_bytes(ag.at[1, :, cols(k)], up_recv.at[k])
        src = ag.at[1, pl.ds(half, half), cols(k)]
        send(src, ag.at[2, pl.ds(half, half), cols(k)], fwd_send, far_recv.at[k], (0, 0, ny - 1))

    ahead = 2
    for k in range(ahead):
        send_own(k)
    half = t_cnt // 2
    send(xag.at[0], xag.at[nx - 1], xag_send.at[0], xag_recv.at[0], (1, 0, 0))
    send(xag.at[0], xag.at[1], xag_send.at[0], xag_recv.at[1], (nx - 1, 0, 0))

    def x_forward():
        wait_bytes(xag.at[nx - 1], xag_recv.at[0])
        send(xag.at[nx - 1, pl.ds(0, half)], xag.at[2, pl.ds(0, half)], xag_send.at[1], xag_recv.at[2], (1, 0, 0))
        wait_bytes(xag.at[1], xag_recv.at[1])
        send(xag.at[1, pl.ds(half, half)], xag.at[2, pl.ds(half, half)], xag_send.at[1], xag_recv.at[2],
             (nx - 1, 0, 0))

    upper = (lax.broadcasted_iota(jnp.int32, (t_cnt, t_cnt), 0)
             < lax.broadcasted_iota(jnp.int32, (t_cnt, t_cnt), 1)).astype(F32).astype(BF)

    def vec_of(scalars):
        r_io = lax.broadcasted_iota(jnp.int32, (len(scalars), t_cnt), 0)
        v = jnp.zeros((len(scalars), t_cnt), jnp.int32)
        for r, s in enumerate(scalars):
            v = jnp.where(r_io == r, s, v)
        return v

    def chosen(ids, s, evec):
        hit = jnp.zeros(evec.shape, F32)
        for m, u in picks:
            hit = jnp.where(ids[s, m, u:u + 1, :] == evec, 1.0, hit)
        return hit

    def one_hot(key, n):
        m = key.shape[0]
        io = lax.broadcasted_iota(jnp.int32, (m, n, t_cnt), 1).astype(F32)
        return key[:, None, :] == io

    e_disp = []
    for l in range(e_loc):
        for dx in range(nx):
            for dc in range(NC):
                gg, jj = at(dx, dc, 0)
                e_disp.append(gg * e_grp + jj * e_loc + l)
    e_disp = vec_of(e_disp)

    g_lo = vec_of([at(dx, dc, 0)[0] * e_grp for dx in range(nx) for dc in range(NC)])
    hit = jnp.zeros(g_lo.shape, F32)
    for m, u in picks:
        row = ids_ref[m, u:u + 1, :]
        hit = jnp.where((row >= g_lo) & (row < g_lo + e_grp), 1.0, hit)
    key = jnp.where(hit > 0.0, dot(hit.astype(BF), upper), -1.0)
    ft = jnp.where(one_hot(key, cap_g), 1.0, 0.0).astype(BF).reshape(nd * cap_g, t_cnt)
    eye = (lax.broadcasted_iota(jnp.int32, (t_cnt, t_cnt), 0)
           == lax.broadcasted_iota(jnp.int32, (t_cnt, t_cnt), 1)).astype(F32).astype(BF)
    fmat[...] = dot_nt(eye, ft).astype(BF)

    yids[0] = ids_ref[...]
    xids[0] = ids_ref[...]
    xgates[0] = gates_ref[...]

    def split(v, n):
        hi = jnp.floor((v + 0.5) * (1.0 / n))
        return hi, v - hi * n

    blk_o, q_o = split(lax.broadcasted_iota(jnp.int32, (rows, rows), 0).astype(F32), cap_e)
    rest_o, rx_o = split(blk_o, nx)
    rc_o, rj_o = split(rest_o, ny)
    src = ((rx_o * NC + rc_o) * ny + rj_o) * cap_e + q_o
    src_io = lax.broadcasted_iota(jnp.int32, (rows, rows), 1).astype(F32)
    perm[...] = jnp.where(src == src_io, 1.0, 0.0).astype(BF)

    with jax.named_scope('wait_yids'):
        wait_bytes(yids.at[pl.ds(1, ny - 1)], meta_recv.at[0])
    load_w('1_0', w1_hbm.at[0], wa.at[0], wa_sem.at[0])
    load_w('3_0', w3_hbm.at[0], wa.at[1], wa_sem.at[1])
    for s in range(ny):
        hit = chosen(yids, s, e_disp)
        key = jnp.where(hit > 0.0, dot(hit.astype(BF), upper) + s * cap_e, -1.0)
        for l in range(e_loc):
            oh = jnp.where(one_hot(key[l * nd:(l + 1) * nd], ny * cap_e), 1.0, 0.0)
            smat[l, :, s * t_cnt:(s + 1) * t_cnt] = oh.astype(BF).reshape(rows, t_cnt)

    col_vecs = []
    for rg in range(NC):
        e_vec = []
        for dj in range(ny):
            for l in range(e_loc):
                gg, jj = at(0, rg, dj)
                e_vec.append(gg * e_grp + jj * e_loc + l)
        col_vecs.append(vec_of(e_vec))

    def col_key(rg, s):
        hit = chosen(xids, s, col_vecs[rg])
        return hit, jnp.where(hit > 0.0, dot(hit.astype(BF), upper) + s * cap_e, -1.0)

    with jax.named_scope('wait_xids'):
        wait_bytes(xids.at[pl.ds(1, nx - 1)], meta_recv.at[1])
    for s in range(nx):
        keys = [col_key(rg, s)[1] for rg in range(NC)]
        for l in range(e_loc):
            key = jnp.concatenate([keys[rg][dj * e_loc + l:dj * e_loc + l + 1]
                                   for rg in range(NC) for dj in range(ny)], axis=0)
            oh = jnp.where(one_hot(key, nx * cap_e), 1.0, 0.0)
            smata[l, :, s * t_cnt:(s + 1) * t_cnt] = oh.astype(BF).reshape(rows, t_cnt)

    def select_b(l, k):
        with jax.named_scope('select#l=%d,k=%d' % (l, k)):
            r = dot(smat[l], ag[:, :, cols(k)].reshape(ny * t_cnt, bk[k][1])).astype(BF)
            r = r.reshape(nd, ny * cap_e, bk[k][1])
            sel[l, :, :, cols(k)] = r
            xin[l, 0, :, cols(k)] = r[0]
            for dx, dc, _ in far_first:
                slot = ((nx - dx) % nx) * NC + dc
                send(sel.at[l, dx * NC + dc, :, cols(k)], xin.at[l, slot, :, cols(k)],
                     disp_send.at[l], disp_recv.at[l, k], (dx, dc, 0))

    def select_a(l):
        with jax.named_scope('select_a#l=%d' % l):
            r = dot(smata[l], xag[...].reshape(nx * t_cnt, aw)).astype(BF).reshape(NC * ny, nx * cap_e, aw)
            sela[l] = r
            xa[l, 0] = r[0]
            for _, dc, dj in col_far_first:
                slot = dc * ny + (ny - dj) % ny
                send(sela.at[l, dc * ny + dj], xa.at[l, slot], dispa_send.at[l], disp_recv.at[l, nk], (0, dc, dj))

    slots = {0: (0, 1), 1: (2, 0)}

    def up_proj(l, k, first=False, last=False):
        s1, s3 = slots[l]
        via_x = k < nk
        with jax.named_scope('wait_rows#l=%d,k=%d' % (l, k)):
            if via_x:
                wait_bytes(xin.at[l, pl.ds(1, nd - 1), :, cols(k)], disp_recv.at[l, k])
            else:
                wait_bytes(xa.at[l, pl.ds(1, NC * ny - 1)], disp_recv.at[l, k])
        if first:
            with jax.named_scope('wait_w13#l=%d' % l):
                wcopies['1_%d' % l].wait()
                wcopies['3_%d' % l].wait()
        with jax.named_scope('h#l=%d,k=%d' % (l, k)):
            if via_x:
                w = bk[k][1]
                xp[:, 0:w] = dot(perm[...], xin[l, :, :, cols(k)].reshape(rows, w)).astype(BF)
            nw = ff // 2

            def body(n, carry):
                cs = pl.ds(pl.multiple_of(n * nw, nw), nw)
                if via_x:
                    xr, kr = xp[:, 0:w], cols(k)
                else:
                    xr, kr = xa[l].reshape(rows, aw), pl.ds(bw, aw)
                d1 = dot(xr, wa[s1, kr, cs])
                d3 = dot(xr, wa[s3, kr, cs])
                if not first:
                    d1 = d1 + h1[:, cs]
                    d3 = d3 + h3[:, cs]
                if last:
                    act[:, cs] = (jax.nn.silu(d1) * d3).astype(BF)
                else:
                    h1[:, cs] = d1
                    h3[:, cs] = d3
                return carry

            lax.fori_loop(0, ff // nw, body, 0)

    def far(k):
        with jax.named_scope('wait_far#k=%d' % k):
            wait_bytes(ag.at[2, :, cols(k)], far_recv.at[k])

    for k in range(nk):
        forward(k)
        if k + ahead < nk:
            send_own(k + ahead)
        if k == 1:
            with jax.named_scope('x_forward'):
                x_forward()
        if k >= 1:
            far(k - 1)
            select_b(0, k - 1)
    load_w('2_0', w2_hbm.at[0], wb, wb_sem.at[0])
    load_w('1_1', w1_hbm.at[1], wa.at[2], wa_sem.at[2])
    with jax.named_scope('wait_xfar'):
        wait_bytes(xag.at[2], xag_recv.at[2])
    select_a(0)
    far(nk - 1)
    select_b(0, nk - 1)
    up_proj(0, 0, first=True)
    select_a(1)
    up_proj(0, 1)
    select_b(1, 0)
    for k in range(2, nk - 1):
        up_proj(0, k)
    up_proj(0, nk)
    up_proj(0, nk - 1, last=True)
    load_w('3_1', w3_hbm.at[1], wa.at[0], wa_sem.at[0])

    ck = [(o, min(nw2 // 2, d_model - o)) for o in range(0, d_model, nw2 // 2)]
    o_last, w_last = ck.pop()
    ck += [(o_last, w_last // 2), (o_last + w_last // 2, w_last // 2)]

    held = [len(ck) - 2, len(ck) - 1]

    def give_back(l, i):
        cs = pl.ds(*ck[i])
        for _, dc, dj in col_far_first:
            slot = dc * ny + (ny - dj) % ny
            send(out.at[l, dc * ny + dj, :, cs], eb.at[slot, l, :, cs],
                 comb_send.at[l], comb_recv.at[l, i], (0, dc, dj))

    def down_proj(l, between=()):
        between = list(between)
        with jax.named_scope('wait_w2#l=%d' % l):
            wcopies['2_%d' % l].wait()
        for o0 in range(0, d_model, nw2):
            wide = pl.ds(o0, nw2)
            with jax.named_scope('w2#l=%d,o=%d' % (l, o0)):
                o = dot(act[...], wb[:, wide]).astype(BF).reshape(NC * ny, nx * cap_e, nw2)
                out[l, :, :, wide] = o
                eb[0, l, :, wide] = o[0]
            for i, (c0, ow) in enumerate(ck):
                if o0 <= c0 < o0 + nw2 and not (l == 0 and i in held):
                    give_back(l, i)
            if between:
                between.pop(0)()

    down_proj(0, [functools.partial(select_b, 1, k) for k in range(1, nk)])
    load_w('2_1', w2_hbm.at[1], wb, wb_sem.at[0])

    up_proj(1, nk, first=True)
    for k in range(nk):
        up_proj(1, k, last=k == nk - 1)
    down_proj(1, [lambda: [give_back(0, i) for i in held]])

    with jax.named_scope('wait_gates'):
        wait_bytes(xgates.at[pl.ds(1, nx - 1)], meta_recv.at[2])
    for rg in range(NC):
        e_vec = col_vecs[rg]
        gs_parts = []
        w_parts = [[], [], []]
        for s in range(nx):
            hit, key = col_key(rg, s)
            gate = jnp.zeros(e_vec.shape, F32)
            for m, u in picks:
                gate = jnp.where(xids[s, m, u:u + 1, :] == e_vec, xgates[s, m, u:u + 1, :], gate)
            any_hit = jnp.max(hit, axis=0, keepdims=True)
            g_hit = jnp.broadcast_to(any_hit, hit.shape)
            g_rank = dot(g_hit.astype(BF), upper)[0:1, :]
            g_key = jnp.where(any_hit > 0.0, g_rank + s * cap_g, -1.0)
            g_io = lax.broadcasted_iota(jnp.int32, (nx * cap_g, t_cnt), 0).astype(F32)
            gs_parts.append(jnp.where(g_key == g_io, 1.0, 0.0).astype(BF))
            g1 = gate.astype(BF)
            rest = gate - g1.astype(F32)
            g2 = rest.astype(BF)
            g3 = (rest - g2.astype(F32)).astype(BF)
            oh = one_hot(key, nx * cap_e)
            for part, gp in zip(w_parts, (g1, g2, g3)):
                w = jnp.where(oh, gp.astype(F32)[:, None, :], 0.0)
                part.append(w.astype(BF).reshape(e_grp * nx * cap_e, t_cnt))
        gs = jnp.concatenate(gs_parts, axis=1)
        n_g = nx * cap_g
        for i in range(3):
            w = jnp.concatenate(w_parts[i], axis=1)
            cmat[rg, i * n_g:(i + 1) * n_g, :] = dot_nt(gs, w).astype(BF)

    def merge(i):
        n_g = nx * cap_g
        cs, ow = pl.ds(*ck[i]), ck[i][1]
        for l in range(e_loc):
            with jax.named_scope('wait_comb#l=%d,i=%d' % (l, i)):
                wait_bytes(eb.at[pl.ds(1, NC * ny - 1), l, :, cs], comb_recv.at[l, i])
        with jax.named_scope('merge#i=%d' % i):
            for rg in range(NC):
                e = eb[rg * ny:(rg + 1) * ny, :, :, cs].reshape(ny * e_loc * nx * cap_e, ow)
                r = dot(cmat[rg], e)
                r = (r[0:n_g] + r[n_g:2 * n_g] + r[2 * n_g:3 * n_g]).astype(BF).reshape(nx, cap_g, ow)
                gsum[:, rg, :, cs] = r
                grec[0, rg, :, cs] = r[0]
            for dx in sorted(range(1, nx), key=lambda d: -min(d, nx - d)):
                send(gsum.at[dx, :, :, cs], grec.at[nx - dx, :, :, cs], fin_send, fin_recv, (dx, 0, 0))

    for i in range(len(ck)):
        merge(i)
    with jax.named_scope('wait_fin'):
        wait_bytes(grec.at[pl.ds(1, nx - 1)], fin_recv)

    wait_bytes(yids.at[pl.ds(1, ny - 1)], meta_send.at[0])
    wait_bytes(xids.at[pl.ds(1, nx - 1)], meta_send.at[1])
    wait_bytes(xgates.at[pl.ds(1, nx - 1)], meta_send.at[2])
    wait_bytes(ag.at[pl.ds(0, 2)], own_send)
    wait_bytes(ag.at[0], fwd_send)
    wait_bytes(xag.at[pl.ds(0, 2)], xag_send.at[0])
    wait_bytes(xag.at[0], xag_send.at[1])
    for l in range(e_loc):
        wait_bytes(sel.at[l, pl.ds(1, nd - 1)], disp_send.at[l])
        wait_bytes(sela.at[l, pl.ds(1, NC * ny - 1)], dispa_send.at[l])
        wait_bytes(out.at[l, pl.ds(1, NC * ny - 1)], comb_send.at[l])
    wait_bytes(gsum.at[pl.ds(1, nx - 1)], fin_send)


def solution(mesh):
    n_grp = mesh.shape['grp']
    ny = mesh.shape['ing']
    nx = n_grp // NC
    row_spec = P(('dp', 'grp', 'ing'))
    exp_spec = P(('grp', 'ing'))

    def local_fn(tokens, expert_ids, gate_vals, w_one, w_three, w_two):
        t_cnt, d_model = tokens.shape
        m_groups, per_group = expert_ids.shape[1:]
        e_loc, _, ff = w_one.shape
        e_grp = e_loc * ny
        cap_g = (t_cnt * m_groups + n_grp - 1) // n_grp
        cap_e = (cap_g * per_group + e_grp - 1) // e_grp
        cw, aw, nw2 = 512, 768, 512
        bw = d_model - aw
        nk = (bw + cw - 1) // cw
        ni = d_model // (nw2 // 2) + 1
        rows = n_grp * ny * cap_e
        dims = (t_cnt, d_model, ff, nx, ny, e_loc, e_grp, cap_g, cap_e, cw, aw, nw2)

        ids_t = jnp.transpose(expert_ids, (1, 2, 0))
        gate_t = jnp.transpose(gate_vals, (1, 2, 0))

        vm, dma = pltpu.VMEM, pltpu.SemaphoreType.DMA
        hbm = pl.BlockSpec(memory_space=pltpu.HBM)
        vmem = pl.BlockSpec(memory_space=pltpu.VMEM)
        blk = nx * cap_e
        sums, pick = pl.pallas_call(
            functools.partial(moe_kernel, dims),
            out_shape=[vm((nx, NC, cap_g, d_model), BF), vm((t_cnt, n_grp * cap_g), BF)],
            in_specs=[hbm, vmem, vmem, hbm, hbm, hbm],
            out_specs=[vmem, vmem],
            scratch_shapes=[
                vm((3, d_model, ff), BF), vm((ff, d_model), BF),
                vm((ny, t_cnt, bw), BF), vm((nx, t_cnt, aw), BF),
                vm((ny,) + ids_t.shape, jnp.int32), vm((nx,) + ids_t.shape, jnp.int32), vm((nx,) + ids_t.shape, F32),
                vm((e_loc, n_grp, ny * cap_e, bw), BF), vm((e_loc, NC * ny, blk, aw), BF),
                vm((e_loc, n_grp, ny * cap_e, bw), BF), vm((e_loc, NC * ny, blk, aw), BF),
                vm((rows, cw), BF), vm((rows, ff), F32), vm((rows, ff), F32), vm((rows, ff), BF),
                vm((e_loc, NC * ny, blk, d_model), BF), vm((NC * ny, e_loc, blk, d_model), BF),
                vm((nx, NC, cap_g, d_model), BF),
                vm((rows, rows), BF), vm((e_loc, rows, ny * t_cnt), BF), vm((e_loc, rows, nx * t_cnt), BF),
                vm((NC, 3 * nx * cap_g, e_grp * blk), BF),
                dma((3,)), dma((1,)), dma((2,)), dma((3,)), dma((3,)),
                dma, dma, dma((nk,)), dma((nk,)), dma((nk,)),
                dma((2,)), dma((3,)), dma((e_loc,)), dma((e_loc,)), dma((e_loc, nk + 1)),
                dma((e_loc,)), dma((e_loc, ni)), dma, dma,
            ],
            compiler_params=pltpu.CompilerParams(
                collective_id=0, has_side_effects=True, vmem_limit_bytes=64800000),
        )(tokens, ids_t, gate_t, w_one, w_three, w_two)
        sums = sums.reshape(n_grp * cap_g, d_model)
        return jnp.dot(pick, sums, preferred_element_type=F32).astype(BF)

    return jax.shard_map(local_fn, mesh=mesh, in_specs=(row_spec, row_spec, row_spec, exp_spec, exp_spec, exp_spec), out_specs=row_spec, check_vma=False)
```
